256 devices in a mesh: px: 16 (over z, y_hi), py: 16 (over x, y_lo, core).
Axes of the slice: x: 4, y: 4 (y_hi: 2, y_lo: 2; y = y_hi * 2 + y_lo), z: 8, core: 2. Of those that a mesh axis runs over, the one named last changes fastest.
Arguments:
- flow_field: bfloat16 [64, 128, 128, 128], P(None, 'px', 'py'), may hold values from -6 to 6
- cotangent: bfloat16 [64, 128, 128, 128], P(None, 'px', 'py'), may hold values from -6 to 6
- tucker_core: float32 [16, 16, 8, 8, 8], replicated, may hold values from -6 to 6
- in_factor: float32 [64, 16], replicated, may hold values from -0.75 to 0.75
- out_factor: float32 [64, 16], replicated, may hold values from -1.5 to 1.5
- first_factor: float32 [32, 8], replicated, may hold values from -2 to 2
- second_factor: float32 [32, 8], replicated, may hold values from -2 to 2
- third_factor: float32 [32, 8], replicated, may hold values from -2 to 2
Outputs:
- output_field: bfloat16 [64, 128, 128, 128], P(None, 'px', 'py')
- core_grad: float32 [16, 16, 8, 8, 8], replicated
- in_grad: float32 [64, 16], replicated
- out_grad: float32 [64, 16], replicated
- first_grad: float32 [32, 8], replicated
- second_grad: float32 [32, 8], replicated
- third_grad: float32 [32, 8], replicated
The draws below stay inside these ranges and needn't reach their ends.
All inputs are finite; a program needn't handle non-finite values.
Results may differ from the reference program's by a relative error of at most 0.001.
Values sent between devices are 32-bit elements; how exact they have to be, the bound alone decides.
No kernel may reach another device: no remote copies, remote signals or barrier semaphores. Data moves between devices by JAX's collectives and lax.ppermute only.
A program may use at most 128 MiB of HBM per device.

```python
import jax
import jax.numpy as jnp
from jax import lax

C = 64
NX = 128
NY = 128
NZ = 128
M1 = 32
M2 = 32
M3 = 32
RI = 16
RO = 16
R1 = 8
R2 = 8
R3 = 8


def block_scale(rng, extent, cuts, low, high):
    def one(position, shards_of):
        heights = jax.random.uniform(jax.random.fold_in(jax.random.fold_in(rng, 6), position), (shards_of,), jnp.float32, low / len(cuts), high / len(cuts))
        return jnp.repeat(jnp.exp(heights), extent[position] // shards_of).reshape((-1,) + (1,) * (len(extent) - position - 1))

    level = one(*cuts[0])
    for cut in cuts[1:]:
        level = level * one(*cut)
    return level


def centred(rng, shape, width, bound, pieces=(), kind=jnp.bfloat16):
    result = jax.random.normal(rng, shape, jnp.float32) * width
    if len(pieces) > 0:
        result = block_scale(rng, shape, pieces, -0.22, 0.18) * result
    return jnp.clip(result, min=-bound, max=bound).astype(kind)


def setup_inputs(seed: int = 0) -> dict:
    key_list = jax.random.split(jax.random.key(seed), 9)
    flow_field = centred(key_list[0], (C, NX, NY, NZ), 1.0, 6.0, ((1, 16), (2, 16)))
    cotangent = centred(key_list[1], (C, NX, NY, NZ), 1.0, 6.0, ((1, 16), (2, 16)))
    tucker_core = centred(key_list[2], (RI, RO, R1, R2, R3), (0.3 * ((NX * NY * NZ) // (2 * M1 * M2 * M3)) ** 0.5), 6.0, (), jnp.float32)
    in_factor = centred(key_list[3], (C, RI), C ** -0.5, 0.75, (), jnp.float32)
    out_factor = centred(key_list[4], (C, RO), RO ** -0.5, 1.5, (), jnp.float32)
    first_factor = centred(key_list[5], (M1, R1), R1 ** -0.5, 2.0, (), jnp.float32)
    second_factor = centred(key_list[6], (M2, R2), R2 ** -0.5, 2.0, (), jnp.float32)
    third_factor = centred(key_list[7], (M3, R3), R3 ** -0.5, 2.0, (), jnp.float32)
    return dict(flow_field=flow_field, cotangent=cotangent, tucker_core=tucker_core, in_factor=in_factor, out_factor=out_factor, first_factor=first_factor, second_factor=second_factor, third_factor=third_factor)


HIGHEST = lax.Precision.HIGHEST

def kept_index(count, length):
    half_count = count // 2
    return jnp.concatenate([jnp.arange(half_count), jnp.arange(length - half_count, length)]).astype(jnp.int32)

def spectrum(plane):
    whole = jnp.fft.rfftn(plane, axes=(0, 1, 2))
    rows_kept = kept_index(M1, NX)
    cols_kept = kept_index(M2, NY)
    trimmed = whole[rows_kept][:, cols_kept][:, :, :M3]
    return jnp.stack([jnp.real(trimmed), jnp.imag(trimmed)])

def to_grid(modes):
    values = modes[0] + 1j * modes[1]
    whole = jnp.zeros((NX, NY, NZ // 2 + 1), values.dtype)
    rows_kept = kept_index(M1, NX)
    cols_kept = kept_index(M2, NY)
    depth_kept = jnp.arange(M3).astype(jnp.int32)
    whole = whole.at[rows_kept[:, None, None], cols_kept[None, :, None], depth_kept[None, None, :]].set(values)
    return jnp.fft.irfftn(whole, s=(NX, NY, NZ), axes=(0, 1, 2))

def mixing(tucker_core, in_factor, out_factor, first_factor, second_factor, third_factor, spectra):
    partial_core = jnp.einsum('abrst,mt->abrsm', tucker_core, third_factor, precision=HIGHEST)
    partial_core = jnp.einsum('abrsm,ks->abrkm', partial_core, second_factor, precision=HIGHEST)
    kernel = jnp.einsum('abrkm,jr->abjkm', partial_core, first_factor, precision=HIGHEST)
    lifted = jnp.einsum('ia,ipjkm->apjkm', in_factor, spectra, precision=HIGHEST)
    mixed = jnp.einsum('abjkm,apjkm->bpjkm', kernel, lifted, precision=HIGHEST)
    return jnp.einsum('ob,bpjkm->opjkm', out_factor, mixed, precision=HIGHEST)

def reference(flow_field, cotangent, tucker_core, in_factor, out_factor, first_factor, second_factor, third_factor):
    spectra = lax.map(lambda plane: spectrum(plane.astype(jnp.float32)), flow_field)
    weights = jnp.where(jnp.arange(M3) == 0, 1.0, 2.0).astype(jnp.float32)
    inverse_count = 1.0 / (NX * NY * NZ)
    back = lax.map(lambda plane: spectrum(plane.astype(jnp.float32)), cotangent) * (weights * inverse_count)

    def forward(core_arg, in_arg, out_arg, first_arg, second_arg, third_arg):
        return mixing(core_arg, in_arg, out_arg, first_arg, second_arg, third_arg, spectra)
    joined, pullback = jax.vjp(forward, tucker_core, in_factor, out_factor, first_factor, second_factor, third_factor)
    grads = pullback(back)
    output_field = lax.map(lambda modes: to_grid(modes).astype(jnp.bfloat16), joined)
    return (output_field, grads[0], grads[1], grads[2], grads[3], grads[4], grads[5])
```

```python
import functools

import jax
import jax.numpy as jnp
import numpy as np
from jax import lax
from jax.experimental import pallas as pl
from jax.experimental.pallas import tpu as pltpu
from jax.sharding import PartitionSpec as P

N = 128
F32 = jnp.float32
BF16 = jnp.bfloat16
NN = (((1,), (0,)), ((), ()))
NT = (((1,), (1,)), ((), ()))
TN = (((0,), (0,)), ((), ()))


def freq(k):
    return np.where(k < 16, k, k - 32)


def turn(phase, sign):
    angle = 2.0 * np.pi / N * np.mod(phase, N)
    c, s = np.cos(angle), sign * np.sin(angle)
    return np.stack([np.stack([c, s]), np.stack([-s, c])])


def split_table(table):
    hi = np.asarray(table, np.float32).astype(jnp.bfloat16)
    lo = (table - hi.astype(np.float64)).astype(np.float32).astype(jnp.bfloat16)
    return hi, lo


@functools.cache
def tables():
    i2, i8, i16 = np.arange(2), np.arange(8), np.arange(16)
    e2 = np.eye(2)
    z = np.arange(N)
    m = 2 * i16[:, None] + i2[None, :]
    ang = 2.0 * np.pi / N * np.mod(m[:, :, None] * z, N)
    tz = np.stack([np.cos(ang), -np.sin(ang)])
    zf = np.einsum("pdmz,yw->dypmwz", tz, e2).reshape(128, 256)
    zi = zf
    k = 2 * i16[:, None] + i2[None, :]
    y = 8 * i16[None, :, None] + 2 * np.arange(4)[:, None, None] + i2[None, None, :]
    ph = freq(k)[:, :, None, None, None] * y[None, None]
    tf = turn(ph, -1.0)
    yf = np.einsum("pqdkgsy,mn->dkmqgsypn", tf, e2).reshape(128, 512)
    ti = turn(ph, 1.0)
    yi = np.einsum("qpskgdy,mn->gdypmsknq", ti, e2).reshape(512, 128)
    x = 8 * i16[None, :] + i8[:, None]
    phx = x[:, :, None] * freq(np.arange(32))[None, None, :]
    tf = turn(phx, -1.0)
    e4 = np.eye(4).reshape(2, 2, 2, 2)
    xf = np.einsum("qrxsj,kmln->xskmqrlnj", tf, e4).reshape(1024, 256)
    ti = turn(phx, 1.0)
    xi = np.einsum("qrxdj,kmln->qkmjxdlnr", ti, e4).reshape(256, 1024)
    sel = np.zeros((8, 128, 2, 2, 4, 8), np.float32)
    for t in range(8):
        for bh in range(2):
            for mm in range(2):
                for r in range(8):
                    sel[t, bh * 16 + mm * 8 + r, r // 4, bh, r % 4, t] = 1.0
    sel = sel.reshape(1024, 128)
    sy = np.kron(np.eye(64), np.ones((8, 1)))
    out = {}
    for name, table in (("zf", zf), ("yf", yf), ("yi", yi), ("xf", xf), ("xi", xi), ("zi", zi)):
        hi, lo = split_table(table)
        axis = 1 if name in ("xf", "xi", "zi") else 0
        out[name] = np.concatenate([hi, lo], axis=axis) if name != "xf" and name != "xi" else np.stack([hi, lo])
    out["zi"] = np.stack(split_table(zi))
    out["sel"] = sel.astype(jnp.bfloat16)
    out["sy"] = sy.astype(np.float32).astype(jnp.bfloat16)
    return out


def split(v):
    hi = v.astype(BF16)
    return hi, (v - hi.astype(F32)).astype(BF16)


def split3(v):
    hi = v.astype(BF16)
    rest = v - hi.astype(F32)
    mid = rest.astype(BF16)
    return hi, mid, (rest - mid.astype(F32)).astype(BF16)


def mul(a, b, dims=NN):
    return lax.dot_general(a, b, dims, preferred_element_type=F32)


def rows_table(table, v, dims=NN):
    half = table.shape[0] // 2
    hi, lo = split(v)
    both = mul(table, hi, dims)
    return both[:half] + both[half:] + mul(table[:half], lo, dims)


def pick(v, table):
    hi, mid, lo = split3(v)
    return mul(hi, table) + mul(mid, table) + mul(lo, table)


def plane(ref, x):
    return ref[:, x].astype(F32).reshape(512, N).astype(BF16)


def fold_kernel(flow, cot, wk, zf, out, work):
    for f, field in enumerate((flow, cot)):
        w = wk[f]
        for pair in range(4):
            u = jnp.concatenate([plane(field, 2 * pair), plane(field, 2 * pair + 1)], axis=1)
            both = mul(w, u)
            v = both[:128] + both[128:]
            for x2 in range(2):
                row = ((2 * pair + x2) * 2 + f) * 16
                for yy in range(8):
                    work[yy // 2, row : row + 16, (yy % 2) * N : (yy % 2 + 1) * N] = v[
                        yy * 16 : yy * 16 + 16, x2 * N : (x2 + 1) * N
                    ]
    table = zf[...]
    for g in range(4):
        out[:, :, g * 256 : (g + 1) * 256] = rows_table(table, work[g], NT).reshape(16, 8, 256)


def y_kernel(data, yf, out):
    v = data[...].reshape(128, 1024)
    v = jnp.concatenate([v[:, g * 256 : (g + 1) * 256] for g in range(4)], axis=0)
    out[...] = rows_table(yf[...], v).reshape(16, 8, 256)


def prep_kernel(core, pack, kern, flat):
    for a in range(16):
        flat[a * 16 : (a + 1) * 16, :] = core[a].T
    f1, f2, f3 = pack[0:8], pack[8:16], pack[16:24]
    w = jnp.concatenate(
        [f1[r : r + 1] * f2[s : s + 1] * f3 for r in range(8) for s in range(8)], axis=0
    )
    wh, wl = split(w)
    ch, cl = split(flat[...])
    kern[...] = mul(ch, wh) + mul(cl, wh) + mul(ch, wl)


def mode_kernel(data, kern, pack, ex, xf, xi, out, gk):
    v = data[...].reshape(128, 256)
    t = jnp.concatenate([v[:, :128].T, v[:, 128:].T], axis=0)
    t = jnp.concatenate([t[x * 32 : (x + 1) * 32] for x in range(8)], axis=1)
    hi, lo = split(t)
    s = mul(hi, xf[0]) + mul(lo, xf[0]) + mul(hi, xf[1])
    wt = pack[24:25]
    lift = [s[:16, q * N : (q + 1) * N] for q in range(2)]
    back = [s[16:, q * N : (q + 1) * N] * wt for q in range(2)]
    mixed = [jnp.zeros((16, N), F32) for _ in range(2)]
    lows = [[], []]
    grads = []
    for a in range(16):
        k = kern[a * 16 : (a + 1) * 16]
        g = None
        for q in range(2):
            la = lift[q][a : a + 1]
            mixed[q] = mixed[q] + k * la
            lows[q].append(jnp.sum(k * back[q], axis=0, keepdims=True))
            g = back[q] * la if g is None else g + back[q] * la
        grads.append(g)
    low = [jnp.concatenate(rows, axis=0) for rows in lows]
    n = jnp.concatenate(
        [jnp.concatenate([mixed[q] * wt, low[q]], axis=0) for q in range(2)], axis=1
    )
    hi, lo = split(n)
    u = mul(hi, xi[0]) + mul(lo, xi[0]) + mul(hi, xi[1])
    u = jnp.concatenate([u[:, x * N : (x + 1) * N] for x in range(8)], axis=0)
    u = jnp.concatenate([u[:128].T, u[128:].T], axis=1)
    out[:, :, 0:256] = u.reshape(16, 8, 256)
    gall = jnp.concatenate(grads, axis=0)
    gk[...] = gall
    gh, gl = split(gall)
    eh, el = split(ex[...])
    gj = mul(gh, eh) + mul(gl, eh) + mul(gh, el)
    gj = gj.reshape(16, 2, 8, N)
    for a in range(16):
        out[a, :, 256:384] = gj[a, 0] + pltpu.roll(gj[a, 1], 64, 1)


def factor_kernel(gk, flat, pack, place, out):
    gh, gl = split(gk[...])
    ch, cl = split(flat[...])
    gw = mul(ch, gh, TN) + mul(cl, gh, TN) + mul(ch, gl, TN)
    f1, f2, f3 = pack[0:8], pack[8:16], pack[16:24]
    first, second = [None] * 8, [None] * 8
    third = None
    for r in range(8):
        for s in range(8):
            tile = gw[(r * 8 + s) * 8 : (r * 8 + s) * 8 + 8]
            t3 = tile * f3
            one = t3 * f2[s : s + 1]
            two = t3 * f1[r : r + 1]
            tri = tile * (f1[r : r + 1] * f2[s : s + 1])
            first[r] = one if first[r] is None else first[r] + one
            second[s] = two if second[s] is None else second[s] + two
            third = tri if third is None else third + tri
    one = jnp.concatenate([jnp.sum(v, axis=0, keepdims=True) for v in first], axis=0)
    two = jnp.concatenate([jnp.sum(v, axis=0, keepdims=True) for v in second], axis=0)
    out[...] = pick(one, place[0]) + pick(two, place[1]) + pick(third, place[2])


def unmode_kernel(data, yi, f2w, fact, out):
    table = yi[...]
    v = data[:, :, 0:256].reshape(128, 256)
    u = rows_table(table, v)
    for g in range(4):
        out[:, :, g * 256 : (g + 1) * 256] = u[g * 128 : (g + 1) * 128].reshape(16, 8, 256)
    lane = lax.broadcasted_iota(jnp.int32, (8, N), 1)
    extra = fact[...]
    for s in range(8):
        acc = jnp.zeros((8, N), F32)
        for d in range(16):
            acc = acc + data[d, :, 256:384] * f2w[d * 8 + s : d * 8 + s + 1]
        acc = acc + pltpu.roll(acc, N - 16, 1)
        acc = jnp.where(lane < 16, acc, pltpu.roll(acc, N - 48, 1))
        acc = jnp.where(lane < 32, acc, extra)
        out[2 * s, :, 1024:1152] = acc
        out[2 * s + 1, :, 1024:1152] = acc


def space_kernel(data, flow, cot, zi, f3w, sel, sy, out, vout, pacc):
    zh, zl = zi[0], zi[1]
    for g in range(4):
        v = data[:, :, g * 256 : (g + 1) * 256].reshape(128, 256)
        hi, lo = split(v)
        r = mul(hi, zh, TN) + mul(lo, zh, TN) + mul(hi, zl, TN)
        rh, rl = split(r)
        for x in range(8):
            for f in range(2):
                for y2 in range(2):
                    row = (2 * g + y2) * 16
                    src = slice(x * 32 + f * 16, x * 32 + f * 16 + 16)
                    lanes = slice(y2 * N, (y2 + 1) * N)
                    vout[f, row : row + 16, x * N : (x + 1) * N] = rh[src, lanes]
                    vout[f, 128 + row : 128 + row + 16, x * N : (x + 1) * N] = rl[src, lanes]
    ri = lax.broadcasted_iota(jnp.int32, (128, 512), 0) // 16
    ci = lax.broadcasted_iota(jnp.int32, (128, 512), 1) % 8
    same = ri == ci
    res = []
    for f, field in ((1, flow), (0, cot)):
        for pair in range(4):
            u = jnp.concatenate([plane(field, 2 * pair), plane(field, 2 * pair + 1)], axis=1)
            part = mul(vout[f, :, pair * 256 : (pair + 1) * 256], u, NT)
            if pair == 0:
                pacc[...] = part
            else:
                pacc[...] += part
        p = jnp.where(same, pacc[:128] + pacc[128:], 0.0)
        q = p[0:16]
        for yy in range(1, 8):
            q = q + p[yy * 16 : yy * 16 + 16]
        res.append(pick(q, sy[...]))
    both = jnp.concatenate(res, axis=1)
    fact = data[0, :, 1024:1152]
    for d in range(1, 16):
        fact = fact + data[d, :, 1024:1152]
    cols = []
    for t in range(8):
        acc = jnp.zeros((8, N), F32)
        for d in range(16):
            acc = acc + data[d, :, 1024:1152] * f3w[d * 8 + t : d * 8 + t + 1]
        cols.append(acc)
    core = pick(jnp.concatenate(cols, axis=1), sel[...])
    row = jnp.concatenate([both[0:8], both[8:16], fact, core], axis=1)
    for d in range(16):
        out[d] = row


def expand_kernel(vin, wk, out):
    w = wk[...]
    for pair in range(4):
        lanes = slice(pair * 256, (pair + 1) * 256)
        hi = vin[0, 0:128, lanes]
        lo = vin[0, 128:256, lanes]
        u = mul(w, jnp.concatenate([hi, lo, hi], axis=0))
        for x2 in range(2):
            out[:, 2 * pair + x2] = u[:, x2 * N : (x2 + 1) * N].reshape(64, 8, N).astype(BF16)


def gather_kernel(data, half, out, g1, g2, g3):
    total = data[0, :, 0:384]
    for d in range(1, 16):
        total = total + data[d, :, 0:384]
    fact = total[:, 256:384]
    g1[...] = pltpu.roll(fact, N - 32, 1)[:, :32]
    g2[...] = pltpu.roll(fact, N - 64, 1)[:, :32]
    g3[...] = pltpu.roll(fact, N - 96, 1)[:, :32]
    lane = lax.broadcasted_iota(jnp.int32, (8, N), 1)
    keep = half[...]
    mine = []
    for a in range(16):
        c = data[a, :, 384:512] * keep
        mine.append(c + pltpu.roll(c, 64, 1))
    tiles = []
    for bh in range(2):
        for q in range(4):
            tile = jnp.zeros((8, N), F32)
            for i in range(4):
                shift = (32 * i - 32 * bh) % N
                moved = mine[4 * q + i]
                moved = pltpu.roll(moved, shift, 1) if shift else moved
                tile = jnp.where(lane // 32 == i, moved, tile)
            tiles.append(tile)
    row = jnp.concatenate([total[:, 0:256]] + tiles, axis=1)
    for d in range(16):
        out[d] = row


def final_kernel(data, core, gin, gout):
    total = data[0, :, 0:256]
    for d in range(1, 16):
        total = total + data[d, :, 0:256]
    gin[0:8] = total[:, 0:64]
    gin[8:16] = total[:, 128:192]
    gout[0:8] = pltpu.roll(total[:, 0:128], 64, 1)[:, :64]
    gout[8:16] = pltpu.roll(total[:, 128:256], 64, 1)[:, :64]
    for d in range(16):
        s, rh = d // 2, d % 2
        c = jnp.concatenate([data[d, :, 256:768], data[d, :, 768:1280]], axis=0)
        core[:, rh * 4 : rh * 4 + 4, s] = c.T.reshape(16, 4, 8, 16)


def call(kernel, outs, scratch=(), flops=1_000_000):
    many = isinstance(outs, (list, tuple))
    shapes = [jax.ShapeDtypeStruct(*o) for o in outs] if many else jax.ShapeDtypeStruct(*outs.o)
    return pl.pallas_call(
        kernel,
        out_shape=shapes,
        scratch_shapes=list(scratch),
        cost_estimate=pl.CostEstimate(flops=flops, bytes_accessed=1_000_000, transcendentals=0),
        compiler_params=pltpu.CompilerParams(vmem_limit_bytes=48 * 1024 * 1024),
    )


def exchange(v, axis):
    return lax.all_to_all(v, axis, split_axis=0, concat_axis=0, tiled=True)


def halves(v):
    hi = lax.reduce_precision(v, 8, 7)
    return hi.astype(BF16), (v - hi).astype(BF16)


def shards(flow, cot, core, in_factor, out_factor, first, second, third):
    tab = {name: jnp.asarray(value) for name, value in tables().items()}
    px, py = lax.axis_index("px"), lax.axis_index("py")
    eye = jnp.eye(8, dtype=BF16)

    def fold(factor):
        parts = jnp.stack(halves(factor.T))
        return (eye[None, :, None, None, :] * parts[:, None, :, :, None]).reshape(256, 512)

    wk = jnp.stack([fold(in_factor), fold(out_factor)])
    oh, ol = halves(out_factor)
    parts = jnp.stack([oh, oh, ol])
    wk2 = (parts.transpose(1, 0, 2)[:, None, :, None, :] * eye[None, :, None, :, None]).reshape(512, 384)

    o1 = call(fold_kernel, [((16, 8, 1024), F32)], [pltpu.VMEM((4, 256, 256), F32)])(
        flow, cot, wk, tab["zf"]
    )[0]
    r1 = exchange(o1, "py")

    f1t, f2t, f3t = first.T, second.T, third.T
    f2own = lax.dynamic_slice_in_dim(f2t, 2 * px, 2, 1)
    f3own = lax.dynamic_slice_in_dim(f3t, 2 * py, 2, 1)
    shape = (8, 2, 2, 32)
    m = 2 * py + jnp.arange(2)
    weight = jnp.where(m == 0, 1.0, 2.0).astype(F32) * (1.0 / (N * N * N))
    pack = jnp.concatenate(
        [
            jnp.broadcast_to(f1t[:, None, None, :], shape),
            jnp.broadcast_to(f2own[:, :, None, None], shape),
            jnp.broadcast_to(f3own[:, None, :, None], shape),
            jnp.broadcast_to(weight[None, None, :, None], shape),
        ],
        axis=0,
    ).reshape(32, N)
    core_t = core.transpose(0, 2, 3, 4, 1).reshape(16, 512, 16)
    kern, flat = call(prep_kernel, [((256, N), F32), ((256, 512), F32)], flops=100_000_000)(core_t, pack)

    ex = jnp.pad(
        (jnp.eye(4, dtype=F32)[:, None, :, None] * first[None, :, None, :]).reshape(128, 32),
        ((0, 0), (0, 96)),
    )
    f2w = second.reshape(16, 2, 8).transpose(0, 2, 1)[:, :, None, None, :, None]
    f2w = jnp.broadcast_to(f2w, (16, 8, 2, 2, 2, 16)).reshape(128, N)
    f3w = third.reshape(16, 2, 8).transpose(0, 2, 1)[:, :, None, None, :, None]
    f3w = jnp.broadcast_to(f3w, (16, 8, 4, 2, 2, 8)).reshape(128, N)
    f3w = jnp.where(jnp.arange(N)[None, :] < 32, f3w, 0.0)
    lane_in = jnp.arange(N)[:, None]
    lane_out = jnp.arange(N)[None, :]
    place = jnp.stack(
        [
            lane_out == 32 + lane_in % 32,
            lane_out == 64 + 2 * px + lane_in // 64,
            lane_out == 96 + 2 * py + lane_in // 32 % 2,
        ]
    ).astype(BF16)
    half = jnp.broadcast_to((jnp.arange(N) // 64 == py % 2).astype(F32)[None, :], (8, N))

    o2 = call(y_kernel, [((16, 8, 256), F32)])(r1, tab["yf"])[0]
    r2 = exchange(o2, "px")
    o3, gk = call(mode_kernel, [((16, 8, 384), F32), ((256, N), F32)])(
        r2, kern, pack, ex, tab["xf"], tab["xi"]
    )
    r3 = exchange(o3, "px")
    fact = call(factor_kernel, [((8, N), F32)], flops=100_000_000)(gk, flat, pack, place)[0]
    o4 = call(unmode_kernel, [((16, 8, 1152), F32)])(r3, tab["yi"], f2w, fact)[0]
    r4 = exchange(o4, "py")
    o5, v = call(
        space_kernel,
        [((16, 8, 512), F32), ((2, 256, 1024), BF16)],
        [pltpu.VMEM((256, 512), F32)],
    )(r4, flow, cot, tab["zi"], f3w, tab["sel"], tab["sy"])
    r5 = exchange(o5, "px")
    field = call(expand_kernel, [((64, 8, 8, N), BF16)], flops=100_000_000)(v, wk2)[0]
    o6, g1, g2, g3 = call(
        gather_kernel, [((16, 8, 1280), F32), ((8, 32), F32), ((8, 32), F32), ((8, 32), F32)]
    )(r5, half)
    r6 = exchange(o6, "py")
    gcore, gin, gout = call(
        final_kernel, [((16, 8, 8, 8, 16), F32), ((16, 64), F32), ((16, 64), F32)]
    )(r6)
    return (field, gcore.transpose(0, 4, 1, 2, 3), gin.T, gout.T, g1.T, g2.T, g3.T)


def solution(mesh):
    spec = P(None, "px", "py", None)
    return jax.shard_map(
        shards,
        mesh=mesh,
        in_specs=(spec, spec, P(), P(), P(), P(), P(), P()),
        out_specs=(spec, P(), P(), P(), P(), P(), P()),
        check_vma=False,
    )
```

```python
import functools

import jax
import jax.numpy as jnp
import numpy as np
from jax import lax
from jax.experimental import pallas as pl
from jax.experimental.pallas import tpu as pltpu
from jax.sharding import PartitionSpec as P

N = 128
F32 = jnp.float32
BF16 = jnp.bfloat16
NN = (((1,), (0,)), ((), ()))
NT = (((1,), (1,)), ((), ()))
TN = (((0,), (0,)), ((), ()))


def freq(k):
    return np.where(k < 16, k, k - 32)


def turn(phase, sign):
    angle = 2.0 * np.pi / N * np.mod(phase, N)
    c, s = np.cos(angle), sign * np.sin(angle)
    return np.stack([np.stack([c, s]), np.stack([-s, c])])


def split_table(table):
    hi = np.asarray(table, np.float32).astype(jnp.bfloat16)
    lo = (table - hi.astype(np.float64)).astype(np.float32).astype(jnp.bfloat16)
    return hi, lo


@functools.cache
def tables():
    i2, i8, i16 = np.arange(2), np.arange(8), np.arange(16)
    e2 = np.eye(2)
    z = np.arange(N)
    m = 2 * i16[:, None] + i2[None, :]
    ang = 2.0 * np.pi / N * np.mod(m[:, :, None] * z, N)
    tz = np.stack([np.cos(ang), -np.sin(ang)])
    zf = np.einsum("pdmz,yw->dypmwz", tz, e2).reshape(128, 256)
    k = 2 * i16[:, None] + i2[None, :]
    y = 8 * i16[None, :, None] + 2 * np.arange(4)[:, None, None] + i2[None, None, :]
    ph = freq(k)[:, :, None, None, None] * y[None, None]
    tf = turn(ph, -1.0)
    yf = np.einsum("pqdkgsy,mn->dkmqgsypn", tf, e2).reshape(128, 512)
    x = 8 * i16[None, :] + i8[:, None]
    phx = x[:, :, None] * freq(np.arange(32))[None, None, :]
    tf = turn(phx, -1.0)
    e4 = np.eye(4).reshape(2, 2, 2, 2)
    xf = np.einsum("qrxsj,kmln->xskmqrlnj", tf, e4).reshape(1024, 256)
    sel = np.zeros((8, 128, 2, 2, 4, 8), np.float32)
    for t in range(8):
        for bh in range(2):
            for mm in range(2):
                for r in range(8):
                    sel[t, bh * 16 + mm * 8 + r, r // 4, bh, r % 4, t] = 1.0
    sel = sel.reshape(1024, 128)
    sy = np.kron(np.eye(64), np.ones((8, 1)))
    return {
        "zf": np.concatenate(split_table(zf), axis=0),
        "yf": np.concatenate(split_table(yf), axis=0),
        "xf": np.stack(split_table(xf)),
        "sel": sel.astype(jnp.bfloat16),
        "sy": sy.astype(np.float32).astype(jnp.bfloat16),
    }


def split(v):
    hi = v.astype(BF16)
    return hi, (v - hi.astype(F32)).astype(BF16)


def split3(v):
    hi = v.astype(BF16)
    rest = v - hi.astype(F32)
    mid = rest.astype(BF16)
    return hi, mid, (rest - mid.astype(F32)).astype(BF16)


def mul(a, b, dims=NN):
    return lax.dot_general(a, b, dims, preferred_element_type=F32)


def rows_table(table, v, dims=NN):
    half = table.shape[0] // 2
    hi, lo = split(v)
    both = mul(table, hi, dims)
    return both[:half] + both[half:] + mul(table[:half], lo, dims)


def pick(v, table):
    hi, mid, lo = split3(v)
    return mul(hi, table) + mul(mid, table) + mul(lo, table)


def plane(ref, x):
    return ref[:, x].astype(F32).reshape(512, N).astype(BF16)


def spread(factor, sy):
    row = lax.broadcasted_iota(jnp.int32, (128, 512), 0) // 16
    col = lax.broadcasted_iota(jnp.int32, (128, 512), 1) % 8
    wide = [mul(part, sy, NT) for part in split(factor)]
    return [
        jnp.where(row == col, jnp.concatenate([w] * 8, axis=0), 0.0).astype(BF16) for w in wide
    ]


def fold_kernel(flow, cot, fin, fout, sy, zf, yf, out, yout, fields, tin, tout, tsy, tzf, work, sems):
    small = [
        pltpu.make_async_copy(src, dst, sems.at[8 + i])
        for i, (src, dst) in enumerate(((fin, tin), (fout, tout), (sy, tsy), (zf, tzf)))
    ]
    for copy in small:
        copy.start()
    get_yf = pltpu.make_async_copy(yf, yout, sems.at[12])
    large = []
    for f, field in enumerate((flow, cot)):
        for part in range(4):
            rows = pl.ds(16 * part, 16)
            copy = pltpu.make_async_copy(
                field.at[rows], fields.at[f, rows], sems.at[4 * f + part]
            )
            copy.start()
            large.append(copy)
    get_yf.start()
    for copy in small:
        copy.wait()
    for f, factor in enumerate((tin, tout)):
        w = jnp.concatenate(spread(factor[...], tsy[...]), axis=0)
        for copy in large[4 * f : 4 * f + 4]:
            copy.wait()
        for pair in range(4):
            u = jnp.concatenate(
                [plane(fields.at[f], 2 * pair), plane(fields.at[f], 2 * pair + 1)], axis=1
            )
            both = mul(w, u)
            v = both[:128] + both[128:]
            for x2 in range(2):
                row = ((2 * pair + x2) * 2 + f) * 16
                for yy in range(8):
                    work[yy // 2, row : row + 16, (yy % 2) * N : (yy % 2 + 1) * N] = v[
                        yy * 16 : yy * 16 + 16, x2 * N : (x2 + 1) * N
                    ]
    table = tzf[...]
    for g in range(4):
        out[:, :, g * 256 : (g + 1) * 256] = rows_table(table, work[g], NT).reshape(16, 8, 256)
    get_yf.wait()


def y_kernel(data, yf, out):
    v = data[...].reshape(128, 1024)
    v = jnp.concatenate([v[:, g * 256 : (g + 1) * 256] for g in range(4)], axis=0)
    out[...] = rows_table(yf[...], v).reshape(16, 8, 256)


def lanes(shape):
    return lax.broadcasted_iota(jnp.int32, shape, 0), lax.broadcasted_iota(jnp.int32, shape, 1)


def marks(cond):
    return jnp.where(cond, 1.0, 0.0).astype(BF16)


def prep_kernel(core, f1t, f2t, f3t, xf, kern, flat, xbuf, pack, ex, f2w, f3w, sem):
    get = pltpu.make_async_copy(xf, xbuf, sem)
    get.start()
    px, py = lax.axis_index("px"), lax.axis_index("py")
    row, lane = lanes((32, N))
    f1 = pick(f1t[...], marks(row == lane % 32))
    f2 = pick(f2t[...], marks(row == 2 * px + lane // 64))
    f3 = pick(f3t[...], marks(row == 2 * py + lane // 32 % 2))
    pack[0:8], pack[8:16], pack[16:24] = f1, f2, f3
    row, lane = lanes((8, N))
    pack[24:32] = jnp.where((py == 0) & (lane // 32 % 2 == 0), 1.0, 2.0) * (1.0 / (N * N * N))
    spread_r = marks(row == lane % 8)
    parts = split3(f1)
    wide = mul(parts[0], spread_r, TN) + mul(parts[1], spread_r, TN) + mul(parts[2], spread_r, TN)
    row, lane = lanes((N, N))
    ex[...] = jnp.where(row // 32 == lane // 8, wide, 0.0)
    for a in range(16):
        flat[a * 16 : (a + 1) * 16, :] = core[a].T
    w = jnp.concatenate(
        [f1[r : r + 1] * f2[s : s + 1] * f3 for r in range(8) for s in range(8)], axis=0
    )
    row, col = lanes((32, 16 * N))
    block, lane = col // N, col % N
    wide2 = pick(f2t[...], marks(row == 2 * block + lane // 16 % 2))
    wide3 = pick(f3t[...], marks((row == 2 * block + lane // 8 % 2) & (lane < 32)))
    for d in range(16):
        f2w[d * 8 : d * 8 + 8] = wide2[:, d * N : (d + 1) * N]
        f3w[d * 8 : d * 8 + 8] = wide3[:, d * N : (d + 1) * N]
    wh, wl = split(w)
    ch, cl = split(flat[...])
    kern[...] = mul(ch, wh) + mul(cl, wh) + mul(ch, wl)
    get.wait()


def mode_kernel(data, kern, pack, ex, xf, out, gk):
    v = data[...].reshape(128, 256)
    t = jnp.concatenate([v[:, :128].T, v[:, 128:].T], axis=0)
    t = jnp.concatenate([t[x * 32 : (x + 1) * 32] for x in range(8)], axis=1)
    hi, lo = split(t)
    s = mul(hi, xf[0]) + mul(lo, xf[0]) + mul(hi, xf[1])
    wt = pack[24:25]
    lift = [s[:16, q * N : (q + 1) * N] for q in range(2)]
    back = [s[16:, q * N : (q + 1) * N] * wt for q in range(2)]
    mixed = [jnp.zeros((16, N), F32) for _ in range(2)]
    lows = [[], []]
    grads = []
    for a in range(16):
        k = kern[a * 16 : (a + 1) * 16]
        g = None
        for q in range(2):
            la = lift[q][a : a + 1]
            mixed[q] = mixed[q] + k * la
            lows[q].append(jnp.sum(k * back[q], axis=0, keepdims=True))
            g = back[q] * la if g is None else g + back[q] * la
        grads.append(g)
    low = [jnp.concatenate(rows, axis=0) for rows in lows]
    gall = jnp.concatenate(grads, axis=0)
    gk[...] = gall
    n = jnp.concatenate(
        [jnp.concatenate([mixed[q] * wt, low[q]], axis=0) for q in range(2)], axis=1
    )
    hi, lo = split(n)
    u = mul(hi, xf[0], NT) + mul(lo, xf[0], NT) + mul(hi, xf[1], NT)
    u = jnp.concatenate([u[:, x * N : (x + 1) * N] for x in range(8)], axis=0)
    u = jnp.concatenate([u[:128].T, u[128:].T], axis=1)
    out[:, :, 0:256] = u.reshape(16, 8, 256)
    gh, gl = split(gall)
    eh, el = split(ex[...])
    gj = mul(gh, eh) + mul(gl, eh) + mul(gh, el)
    gj = gj.reshape(16, 2, 8, N)
    for a in range(16):
        out[a, :, 256:384] = gj[a, 0] + pltpu.roll(gj[a, 1], 64, 1)


def factor_grads(gk, flat, pack):
    gh, gl = split(gk[...])
    ch, cl = split(flat[...])
    gw = mul(ch, gh, TN) + mul(cl, gh, TN) + mul(ch, gl, TN)
    f1, f2, f3 = pack[0:8], pack[8:16], pack[16:24]
    first, second = [None] * 8, [None] * 8
    third = None
    for r in range(8):
        for s in range(8):
            tile = gw[(r * 8 + s) * 8 : (r * 8 + s) * 8 + 8]
            t3 = tile * f3
            one = t3 * f2[s : s + 1]
            two = t3 * f1[r : r + 1]
            tri = tile * (f1[r : r + 1] * f2[s : s + 1])
            first[r] = one if first[r] is None else first[r] + one
            second[s] = two if second[s] is None else second[s] + two
            third = tri if third is None else third + tri
    one = jnp.concatenate([jnp.sum(v, axis=0, keepdims=True) for v in first], axis=0)
    two = jnp.concatenate([jnp.sum(v, axis=0, keepdims=True) for v in second], axis=0)
    src, dst = lanes((N, N))
    total = jnp.zeros((8, N), F32)
    for v, lane in ((one, 96 + src % 32), (two, 64 + src // 64), (third, 66 + src // 32 % 2)):
        total = total + pick(v, marks(dst == lane))
    return total


def unmode_kernel(data, yf, f2w, gk, flat, pack, out, fact):
    hi, lo = split(data[:, :, 0:256].reshape(128, 256))
    u = mul(yf[...], jnp.concatenate([hi, hi], axis=0), TN) + mul(yf[:128], lo, TN)
    for g in range(4):
        out[:, :, g * 256 : (g + 1) * 256] = u[g * 128 : (g + 1) * 128].reshape(16, 8, 256)
    lane = lax.broadcasted_iota(jnp.int32, (8, N), 1)
    extra = factor_grads(gk, flat, pack)
    fact[...] = extra
    for s in range(8):
        acc = jnp.zeros((8, N), F32)
        for d in range(16):
            acc = acc + data[d, :, 256:384] * f2w[d * 8 + s : d * 8 + s + 1]
        acc = acc + pltpu.roll(acc, N - 16, 1)
        acc = jnp.where(lane < 16, acc, pltpu.roll(acc, N - 48, 1))
        acc = jnp.where(lane < 32, acc, extra)
        out[2 * s, :, 1024:1152] = acc
        out[2 * s + 1, :, 1024:1152] = acc


def space_kernel(
    data, zf, f3w, fact_in, sy, fout, flow, cot, sel, out, result, fields, vout, obuf, pacc, tsel, sems
):
    loads = []
    for f, field in enumerate((flow, cot)):
        for part in range(4):
            rows = pl.ds(16 * part, 16)
            load = pltpu.make_async_copy(
                field.at[rows], fields.at[f, rows], sems.at[4 * f + part]
            )
            load.start()
            loads.append(load)
    get_sel = pltpu.make_async_copy(sel, tsel, sems.at[8])
    get_sel.start()
    zh, zl = zf[:128], zf[128:]
    for g in range(4):
        v = data[:, :, g * 256 : (g + 1) * 256].reshape(128, 256)
        hi, lo = split(v)
        r = mul(hi, zh, TN) + mul(lo, zh, TN) + mul(hi, zl, TN)
        rh, rl = split(r)
        for x in range(8):
            for f in range(2):
                for y2 in range(2):
                    row = (2 * g + y2) * 16
                    src = slice(x * 32 + f * 16, x * 32 + f * 16 + 16)
                    cols = slice(y2 * N, (y2 + 1) * N)
                    vout[f, row : row + 16, x * N : (x + 1) * N] = rh[src, cols]
                    vout[f, 128 + row : 128 + row + 16, x * N : (x + 1) * N] = rl[src, cols]
    brow, bcol = lanes((16, N))
    repeat = marks(brow == bcol % 16)
    orow, ocol = lanes((512, N))
    wide = [
        jnp.where(orow % 8 == ocol // 16, mul(sy[...], mul(part, repeat, TN).astype(BF16)), 0.0)
        for part in split(fout[...])
    ]
    hi, lo = wide[0].astype(BF16), wide[1].astype(BF16)
    w = jnp.concatenate([hi, hi, lo], axis=1)
    for pair in range(4):
        cols = slice(pair * 256, (pair + 1) * 256)
        hi = vout[0, 0:128, cols]
        lo = vout[0, 128:256, cols]
        u = mul(w, jnp.concatenate([hi, lo, hi], axis=0))
        for x2 in range(2):
            obuf[:, 2 * pair + x2] = u[:, x2 * N : (x2 + 1) * N].reshape(64, 8, N).astype(BF16)
    puts = []
    for part in range(4):
        rows = pl.ds(16 * part, 16)
        put = pltpu.make_async_copy(obuf.at[rows], result.at[rows], sems.at[9 + part])
        put.start()
        puts.append(put)
    fact = data[0, :, 1024:1152]
    for d in range(1, 16):
        fact = fact + data[d, :, 1024:1152]
    cols = []
    for t in range(8):
        acc = jnp.zeros((8, N), F32)
        for d in range(16):
            acc = acc + data[d, :, 1024:1152] * f3w[d * 8 + t : d * 8 + t + 1]
        cols.append(acc)
    lane = lanes((8, N))[1]
    get_sel.wait()
    core = pick(jnp.concatenate(cols, axis=1), tsel[...])
    core = jnp.where(lane // 64 == lax.axis_index("py") % 2, core, 0.0)
    core = core + pltpu.roll(core, 64, 1)
    fact = jnp.where((lane == 66) | (lane == 67), fact_in[...], fact)
    last = jnp.where(lane < 64, core, fact)
    ri, ci = lanes((128, 512))
    same = ri // 16 == ci % 8
    res = []
    for f in range(2):
        field = fields.at[f]
        for load in loads[4 * f : 4 * f + 4]:
            load.wait()
        for pair in range(4):
            u = jnp.concatenate([plane(field, 2 * pair), plane(field, 2 * pair + 1)], axis=1)
            part = mul(vout[1 - f, :, pair * 256 : (pair + 1) * 256], u, NT)
            if pair == 0:
                pacc[...] = part
            else:
                pacc[...] += part
        p = jnp.where(same, pacc[:128] + pacc[128:], 0.0)
        q = p[0:16]
        for yy in range(1, 8):
            q = q + p[yy * 16 : yy * 16 + 16]
        res.append(pick(q, sy[...]))
    both = jnp.concatenate(res, axis=1)
    row = jnp.concatenate([both[0:8], both[8:16], last], axis=1)
    for d in range(16):
        out[d] = row
    for put in puts:
        put.wait()


def gather_kernel(data, out, g1, g2):
    total = data[0]
    for d in range(1, 16):
        total = total + data[d]
    fact = total[:, 256:384]
    g1[...] = pltpu.roll(fact, N - 96, 1)[:, :32]
    lane = lax.broadcasted_iota(jnp.int32, (8, N), 1)
    second = jnp.zeros((8, N), F32)
    for d in range(16):
        moved = pltpu.roll(data[d, :, 256:384], (2 * d - 64) % N, 1)
        second = jnp.where(lane // 2 == d, moved, second)
    g2[...] = second[:, :32]
    tiles = []
    for bh in range(2):
        for q in range(4):
            tile = jnp.zeros((8, N), F32)
            for i in range(4):
                shift = (32 * i - 32 * bh) % N
                moved = data[4 * q + i, :, 256:384]
                moved = pltpu.roll(moved, shift, 1) if shift else moved
                tile = jnp.where(lane // 32 == i, moved, tile)
            tiles.append(tile)
    row = jnp.concatenate([total[:, 0:256]] + tiles + [fact], axis=1)
    for d in range(16):
        out[d] = row


def final_kernel(data, core, gin, gout, g3, buf, sems):
    sends = []
    for q in range(4):
        for d in range(16):
            lo, hi = 256 + q * N, 768 + q * N
            c = jnp.concatenate([data[d, :, lo : lo + N], data[d, :, hi : hi + N]], axis=0)
            rows = slice(d % 2 * 4, d % 2 * 4 + 4)
            buf[4 * q : 4 * q + 4, rows, d // 2] = c.T.reshape(4, 4, 8, 16)
        part = pl.ds(4 * q, 4)
        send = pltpu.make_async_copy(buf.at[part], core.at[part], sems.at[q])
        send.start()
        sends.append(send)
    total = data[0, :, 0:256]
    for d in range(1, 16):
        total = total + data[d, :, 0:256]
    gin[0:8] = total[:, 0:64]
    gin[8:16] = total[:, 128:192]
    gout[0:8] = pltpu.roll(total[:, 0:128], 64, 1)[:, :64]
    gout[8:16] = pltpu.roll(total[:, 128:256], 64, 1)[:, :64]
    lane = lax.broadcasted_iota(jnp.int32, (8, N), 1)
    third = jnp.zeros((8, N), F32)
    for d in range(16):
        moved = pltpu.roll(data[d, :, 1280:1408], (2 * d - 66) % N, 1)
        third = jnp.where(lane // 2 == d, moved, third)
    g3[...] = third[:, :32]
    for send in sends:
        send.wait()


VM = pl.BlockSpec(memory_space=pltpu.VMEM)
HB = pl.BlockSpec(memory_space=pltpu.HBM)
DMA = pltpu.SemaphoreType.DMA


def call(kernel, ins, outs, scratch=(), flops=1_000_000, vmem=12):
    shapes = [
        pltpu.HBM(*o[:2]) if len(o) > 2 and o[2] is HB
        else jax.ShapeDtypeStruct(*o)
        for o in outs
    ]
    run = pl.pallas_call(
        kernel,
        out_shape=shapes,
        in_specs=[VM] * ins[0] + [HB] * ins[1],
        out_specs=[o[2] if len(o) > 2 else VM for o in outs],
        scratch_shapes=list(scratch),
        cost_estimate=pl.CostEstimate(flops=flops, bytes_accessed=1_000_000, transcendentals=0),
        compiler_params=pltpu.CompilerParams(vmem_limit_bytes=vmem * 1024 * 1024),
    )

    def placed(*args):
        far = [pltpu.with_memory_space_constraint(v, pltpu.HBM) for v in args[ins[0] :]]
        return run(*args[: ins[0]], *far)

    return placed


def exchange(v, axis):
    return lax.all_to_all(v, axis, split_axis=0, concat_axis=0, tiled=True)


def shards(flow, cot, core, in_factor, out_factor, first, second, third):
    tab = {name: jnp.asarray(value) for name, value in tables().items()}
    fin, fout = in_factor.T, out_factor.T

    o1, yf = call(
        fold_kernel,
        (0, 7),
        [((16, 8, 1024), F32), ((256, 512), BF16)],
        [
            pltpu.VMEM((2, 64, 8, 8, N), BF16),
            pltpu.VMEM((16, 64), F32),
            pltpu.VMEM((16, 64), F32),
            pltpu.VMEM((512, 64), BF16),
            pltpu.VMEM((256, 256), BF16),
            pltpu.VMEM((4, 256, 256), F32),
            DMA((13,)),
        ],
    )(flow, cot, fin, fout, tab["sy"], tab["zf"], tab["yf"])
    r1 = exchange(o1, "py")
    r1, core, first, second, third = lax.optimization_barrier((r1, core, first, second, third))
    f1t, f2t, f3t = first.T, second.T, third.T
    core_t = core.transpose(0, 2, 3, 4, 1).reshape(16, 512, 16)
    kern, flat, xf, pack, ex, f2w, f3w = call(
        prep_kernel,
        (4, 1),
        [
            ((256, N), F32),
            ((256, 512), F32),
            ((2, 1024, 256), BF16),
            ((32, N), F32),
            ((N, N), F32),
            ((N, N), F32),
            ((N, N), F32),
        ],
        [DMA],
        flops=100_000_000,
    )(core_t, f1t, f2t, f3t, tab["xf"])
    o2 = call(y_kernel, (2, 0), [((16, 8, 256), F32)])(r1, yf)[0]
    r2 = exchange(o2, "px")
    o3, gk = call(mode_kernel, (5, 0), [((16, 8, 384), F32), ((256, N), F32)])(
        r2, kern, pack, ex, xf
    )
    r3 = exchange(o3, "px")
    o4, fact = call(unmode_kernel, (6, 0), [((16, 8, 1152), F32), ((8, N), F32)])(
        r3, yf, f2w, gk, flat, pack
    )
    r4 = exchange(o4, "py")
    o5, field = call(
        space_kernel,
        (6, 3),
        [((16, 8, 384), F32), ((64, 8, 8, N), BF16, HB)],
        [
            pltpu.VMEM((2, 64, 8, 8, N), BF16),
            pltpu.VMEM((2, 256, 1024), BF16),
            pltpu.VMEM((64, 8, 8, N), BF16),
            pltpu.VMEM((256, 512), F32),
            pltpu.VMEM((1024, N), BF16),
            DMA((13,)),
        ],
    )(r4, tab["zf"], f3w, fact, tab["sy"], fout, flow, cot, tab["sel"])
    r5 = exchange(o5, "px")
    o6, g1, g2 = call(
        gather_kernel, (1, 0), [((16, 8, 1408), F32), ((8, 32), F32), ((8, 32), F32)]
    )(r5)
    r6 = exchange(o6, "py")
    gcore, gin, gout, g3 = call(
        final_kernel,
        (1, 0),
        [((16, 8, 8, 8, 16), F32, HB), ((16, 64), F32), ((16, 64), F32), ((8, 32), F32)],
        [pltpu.VMEM((16, 8, 8, 8, 16), F32), DMA((4,))],
    )(r6)
    return (field, gcore.transpose(0, 4, 1, 2, 3), gin.T, gout.T, g1.T, g2.T, g3.T)


def solution(mesh):
    spec = P(None, "px", "py", None)
    return jax.shard_map(
        shards,
        mesh=mesh,
        in_specs=(spec, spec, P(), P(), P(), P(), P(), P()),
        out_specs=(spec, P(), P(), P(), P(), P(), P()),
        check_vma=False,
    )
```

```python
import functools

import jax
import jax.numpy as jnp
import numpy as np
from jax import lax
from jax.experimental import pallas as pl
from jax.experimental.pallas import tpu as pltpu
from jax.sharding import PartitionSpec as P

N = 128
F32 = jnp.float32
BF16 = jnp.bfloat16
NN = (((1,), (0,)), ((), ()))
NT = (((1,), (1,)), ((), ()))
TN = (((0,), (0,)), ((), ()))


def freq(k):
    return np.where(k < 16, k, k - 32)


def turn(phase, sign):
    angle = 2.0 * np.pi / N * np.mod(phase, N)
    c, s = np.cos(angle), sign * np.sin(angle)
    return np.stack([np.stack([c, s]), np.stack([-s, c])])


def split_table(table):
    hi = np.asarray(table, np.float32).astype(jnp.bfloat16)
    lo = (table - hi.astype(np.float64)).astype(np.float32).astype(jnp.bfloat16)
    return hi, lo


@functools.cache
def tables():
    i2, i8, i16 = np.arange(2), np.arange(8), np.arange(16)
    e2 = np.eye(2)
    z = np.arange(N)
    m = 2 * i16[:, None] + i2[None, :]
    ang = 2.0 * np.pi / N * np.mod(m[:, :, None] * z, N)
    tz = np.stack([np.cos(ang), -np.sin(ang)])
    zf = np.einsum("pdmz,yw->dypmwz", tz, e2).reshape(128, 256)
    k = 2 * i16[:, None] + i2[None, :]
    y = 8 * i16[None, :, None] + 2 * np.arange(4)[:, None, None] + i2[None, None, :]
    ph = freq(k)[:, :, None, None, None] * y[None, None]
    tf = turn(ph, -1.0)
    yf = np.einsum("pqdkgsy,mn->dkmqgsypn", tf, e2).reshape(128, 512)
    x = 8 * i16[None, :] + i8[:, None]
    phx = x[:, :, None] * freq(np.arange(32))[None, None, :]
    tf = turn(phx, -1.0)
    e4 = np.eye(4).reshape(2, 2, 2, 2)
    xf = np.einsum("qrxsj,kmln->xskmqrlnj", tf, e4).reshape(1024, 256)
    sel = np.zeros((8, 128, 2, 2, 4, 8), np.float32)
    for t in range(8):
        for bh in range(2):
            for mm in range(2):
                for r in range(8):
                    sel[t, bh * 16 + mm * 8 + r, r // 4, bh, r % 4, t] = 1.0
    sel = sel.reshape(1024, 128)
    return {
        "zf": np.concatenate(split_table(zf), axis=0),
        "yf": np.concatenate(split_table(yf), axis=0),
        "xf": np.stack(split_table(xf)),
        "sel": sel.astype(jnp.bfloat16),
    }


def split(v):
    hi = v.astype(BF16)
    return hi, (v - hi.astype(F32)).astype(BF16)


def split3(v):
    hi = v.astype(BF16)
    rest = v - hi.astype(F32)
    mid = rest.astype(BF16)
    return hi, mid, (rest - mid.astype(F32)).astype(BF16)


def mul(a, b, dims=NN):
    return lax.dot_general(a, b, dims, preferred_element_type=F32)


def rows_table(table, v, dims=NN):
    half = table.shape[0] // 2
    hi, lo = split(v)
    both = mul(table, hi, dims)
    return both[:half] + both[half:] + mul(table[:half], lo, dims)


def pick(v, table):
    hi, mid, lo = split3(v)
    return mul(hi, table) + mul(mid, table) + mul(lo, table)


def plane(ref, x):
    return ref[:, x].astype(F32).reshape(512, N).astype(BF16)


def sum_y():
    row, col = lanes((512, 64))
    return marks(row // 8 == col)


def spread(factor, sy):
    row = lax.broadcasted_iota(jnp.int32, (128, 512), 0) // 16
    col = lax.broadcasted_iota(jnp.int32, (128, 512), 1) % 8
    wide = [mul(part, sy, NT) for part in split(factor)]
    return [
        jnp.where(row == col, jnp.concatenate([w] * 8, axis=0), 0.0).astype(BF16) for w in wide
    ]


def fold_kernel(flow, cot, fin, fout, zf, yf, out, yout, tout, fields, tin, tzf, work, sems):
    small = [
        pltpu.make_async_copy(src, dst, sems.at[8 + i])
        for i, (src, dst) in enumerate(((fin, tin), (fout, tout), (zf, tzf)))
    ]
    for copy in small:
        copy.start()
    get_yf = pltpu.make_async_copy(yf, yout, sems.at[12])
    large = []
    for f, field in enumerate((flow, cot)):
        for part in range(4):
            rows = pl.ds(16 * part, 16)
            copy = pltpu.make_async_copy(
                field.at[rows], fields.at[f, rows], sems.at[4 * f + part]
            )
            copy.start()
            large.append(copy)
    get_yf.start()
    for copy in small:
        copy.wait()
    sy = sum_y()
    for f, factor in enumerate((tin, tout)):
        w = jnp.concatenate(spread(factor[...], sy), axis=0)
        for copy in large[4 * f : 4 * f + 4]:
            copy.wait()
        for pair in range(4):
            u = jnp.concatenate(
                [plane(fields.at[f], 2 * pair), plane(fields.at[f], 2 * pair + 1)], axis=1
            )
            both = mul(w, u)
            v = both[:128] + both[128:]
            for x2 in range(2):
                row = ((2 * pair + x2) * 2 + f) * 16
                for yy in range(8):
                    work[yy // 2, row : row + 16, (yy % 2) * N : (yy % 2 + 1) * N] = v[
                        yy * 16 : yy * 16 + 16, x2 * N : (x2 + 1) * N
                    ]
    table = tzf[...]
    for g in range(4):
        out[:, :, g * 256 : (g + 1) * 256] = rows_table(table, work[g], NT).reshape(16, 8, 256)
    get_yf.wait()


def y_kernel(data, yf, out):
    v = data[...].reshape(128, 1024)
    v = jnp.concatenate([v[:, g * 256 : (g + 1) * 256] for g in range(4)], axis=0)
    out[...] = rows_table(yf[...], v).reshape(16, 8, 256)


def lanes(shape):
    return lax.broadcasted_iota(jnp.int32, shape, 0), lax.broadcasted_iota(jnp.int32, shape, 1)


def marks(cond):
    return jnp.where(cond, 1.0, 0.0).astype(BF16)


def prep_kernel(
    f1h, f2h, f3h, core, xf, kern, flat, xbuf, pack, ex, f2w, f3w, f1t, f2t, f3t, cbuf, sems
):
    small = [
        pltpu.make_async_copy(src, dst, sems.at[i])
        for i, (src, dst) in enumerate(((f1h, f1t), (f2h, f2t), (f3h, f3t)))
    ]
    loads = [pltpu.make_async_copy(core.at[a], cbuf.at[a], sems.at[4 + a]) for a in range(16)]
    get = pltpu.make_async_copy(xf, xbuf, sems.at[3])
    for copy in small + loads + [get]:
        copy.start()
    for copy in small:
        copy.wait()
    px, py = lax.axis_index("px"), lax.axis_index("py")
    row, lane = lanes((32, N))
    f1 = pick(f1t[...], marks(row == lane % 32))
    f2 = pick(f2t[...], marks(row == 2 * px + lane // 64))
    f3 = pick(f3t[...], marks(row == 2 * py + lane // 32 % 2))
    pack[0:8], pack[8:16], pack[16:24] = f1, f2, f3
    row, lane = lanes((8, N))
    pack[24:32] = jnp.where((py == 0) & (lane // 32 % 2 == 0), 1.0, 2.0) * (1.0 / (N * N * N))
    spread_r = marks(row == lane % 8)
    parts = split3(f1)
    wide = mul(parts[0], spread_r, TN) + mul(parts[1], spread_r, TN) + mul(parts[2], spread_r, TN)
    row, lane = lanes((N, N))
    ex[...] = jnp.where(row // 32 == lane // 8, wide, 0.0)
    w = jnp.concatenate(
        [f1[r : r + 1] * f2[s : s + 1] * f3 for r in range(8) for s in range(8)], axis=0
    )
    row, col = lanes((32, 16 * N))
    block, lane = col // N, col % N
    wide2 = pick(f2t[...], marks(row == 2 * block + lane // 16 % 2))
    wide3 = pick(f3t[...], marks((row == 2 * block + lane // 8 % 2) & (lane < 32)))
    for d in range(16):
        f2w[d * 8 : d * 8 + 8] = wide2[:, d * N : (d + 1) * N]
        f3w[d * 8 : d * 8 + 8] = wide3[:, d * N : (d + 1) * N]
    wh, wl = split(w)
    for a in range(16):
        loads[a].wait()
        flat[a * 16 : (a + 1) * 16, :] = cbuf[a].T
    ch, cl = split(flat[...])
    kern[...] = mul(ch, wh) + mul(cl, wh) + mul(ch, wl)
    get.wait()


def mode_kernel(data, kern, pack, ex, xf, out, gk):
    v = data[...].reshape(128, 256)
    t = jnp.concatenate([v[:, :128].T, v[:, 128:].T], axis=0)
    t = jnp.concatenate([t[x * 32 : (x + 1) * 32] for x in range(8)], axis=1)
    hi, lo = split(t)
    s = mul(hi, xf[0]) + mul(lo, xf[0]) + mul(hi, xf[1])
    wt = pack[24:25]
    lift = [s[:16, q * N : (q + 1) * N] for q in range(2)]
    back = [s[16:, q * N : (q + 1) * N] * wt for q in range(2)]
    mixed = [jnp.zeros((16, N), F32) for _ in range(2)]
    lows = [[], []]
    grads = []
    for a in range(16):
        k = kern[a * 16 : (a + 1) * 16]
        g = None
        for q in range(2):
            la = lift[q][a : a + 1]
            mixed[q] = mixed[q] + k * la
            lows[q].append(jnp.sum(k * back[q], axis=0, keepdims=True))
            g = back[q] * la if g is None else g + back[q] * la
        grads.append(g)
    low = [jnp.concatenate(rows, axis=0) for rows in lows]
    gall = jnp.concatenate(grads, axis=0)
    gk[...] = gall
    n = jnp.concatenate(
        [jnp.concatenate([mixed[q] * wt, low[q]], axis=0) for q in range(2)], axis=1
    )
    hi, lo = split(n)
    u = mul(hi, xf[0], NT) + mul(lo, xf[0], NT) + mul(hi, xf[1], NT)
    u = jnp.concatenate([u[:, x * N : (x + 1) * N] for x in range(8)], axis=0)
    u = jnp.concatenate([u[:128].T, u[128:].T], axis=1)
    out[:, :, 0:256] = u.reshape(16, 8, 256)
    gh, gl = split(gall)
    eh, el = split(ex[...])
    gj = mul(gh, eh) + mul(gl, eh) + mul(gh, el)
    gj = gj.reshape(16, 2, 8, N)
    for a in range(16):
        out[a, :, 256:384] = gj[a, 0] + pltpu.roll(gj[a, 1], 64, 1)


def factor_grads(gk, flat, pack):
    gh, gl = split(gk[...])
    ch, cl = split(flat[...])
    gw = mul(ch, gh, TN) + mul(cl, gh, TN) + mul(ch, gl, TN)
    f1, f2, f3 = pack[0:8], pack[8:16], pack[16:24]
    first, second = [None] * 8, [None] * 8
    third = None
    for r in range(8):
        for s in range(8):
            tile = gw[(r * 8 + s) * 8 : (r * 8 + s) * 8 + 8]
            t3 = tile * f3
            one = t3 * f2[s : s + 1]
            two = t3 * f1[r : r + 1]
            tri = tile * (f1[r : r + 1] * f2[s : s + 1])
            first[r] = one if first[r] is None else first[r] + one
            second[s] = two if second[s] is None else second[s] + two
            third = tri if third is None else third + tri
    one = jnp.concatenate([jnp.sum(v, axis=0, keepdims=True) for v in first], axis=0)
    two = jnp.concatenate([jnp.sum(v, axis=0, keepdims=True) for v in second], axis=0)
    src, dst = lanes((N, N))
    total = jnp.zeros((8, N), F32)
    for v, lane in ((one, 96 + src % 32), (two, 64 + src // 64), (third, 66 + src // 32 % 2)):
        total = total + pick(v, marks(dst == lane))
    return total


def unmode_kernel(data, yf, f2w, gk, flat, pack, out, fact):
    hi, lo = split(data[:, :, 0:256].reshape(128, 256))
    u = mul(yf[...], jnp.concatenate([hi, hi], axis=0), TN) + mul(yf[:128], lo, TN)
    for g in range(4):
        out[:, :, g * 256 : (g + 1) * 256] = u[g * 128 : (g + 1) * 128].reshape(16, 8, 256)
    lane = lax.broadcasted_iota(jnp.int32, (8, N), 1)
    extra = factor_grads(gk, flat, pack)
    fact[...] = extra
    for s in range(8):
        acc = jnp.zeros((8, N), F32)
        for d in range(16):
            acc = acc + data[d, :, 256:384] * f2w[d * 8 + s : d * 8 + s + 1]
        acc = acc + pltpu.roll(acc, N - 16, 1)
        acc = jnp.where(lane < 16, acc, pltpu.roll(acc, N - 48, 1))
        acc = jnp.where(lane < 32, acc, extra)
        out[2 * s, :, 1024:1152] = acc
        out[2 * s + 1, :, 1024:1152] = acc


def core_tile(data, f3w, fact_in, get_sel, tsel):
    fact = data[0, :, 1024:1152]
    for d in range(1, 16):
        fact = fact + data[d, :, 1024:1152]
    cols = []
    for t in range(8):
        acc = jnp.zeros((8, N), F32)
        for d in range(16):
            acc = acc + data[d, :, 1024:1152] * f3w[d * 8 + t : d * 8 + t + 1]
        cols.append(acc)
    lane = lanes((8, N))[1]
    get_sel.wait()
    core = pick(jnp.concatenate(cols, axis=1), tsel[...])
    core = jnp.where(lane // 64 == lax.axis_index("py") % 2, core, 0.0)
    core = core + pltpu.roll(core, 64, 1)
    fact = jnp.where((lane == 66) | (lane == 67), fact_in[...], fact)
    return jnp.where(lane < 64, core, fact)


def space_kernel(
    data, zf, f3w, fact_in, flow, cot, sel, out, vfirst, second, vsecond, tsel, sems
):
    sy = sum_y()
    vout = (vfirst, vsecond)
    get_sel = pltpu.make_async_copy(sel, tsel, sems.at[8])
    get_sel.start()
    loads = []
    for part in range(4):
        rows = pl.ds(16 * part, 16)
        load = pltpu.make_async_copy(cot.at[rows], second.at[rows], sems.at[part])
        load.start()
        loads.append(load)
    zh, zl = zf[:128], zf[128:]
    for g in range(4):
        v = data[:, :, g * 256 : (g + 1) * 256].reshape(128, 256)
        hi, lo = split(v)
        r = mul(hi, zh, TN) + mul(lo, zh, TN) + mul(hi, zl, TN)
        rh, rl = split(r)
        for x in range(8):
            for f in range(2):
                for y2 in range(2):
                    row = (2 * g + y2) * 16
                    src = slice(x * 32 + f * 16, x * 32 + f * 16 + 16)
                    cols = slice(y2 * N, (y2 + 1) * N)
                    vout[f][row : row + 16, x * N : (x + 1) * N] = rh[src, cols]
                    vout[f][128 + row : 128 + row + 16, x * N : (x + 1) * N] = rl[src, cols]
    ri, ci = lanes((128, 512))
    same = ri // 16 == ci % 8
    res = []
    for f, field in enumerate((flow, second)):
        for load in loads if f else ():
            load.wait()
        u = jnp.concatenate([plane(field, x) for x in range(8)], axis=1)
        part = mul(vout[1 - f][...], u, NT)
        p = jnp.where(same, part[:128] + part[128:], 0.0)
        q = p[0:16]
        for yy in range(1, 8):
            q = q + p[yy * 16 : yy * 16 + 16]
        res.append(pick(q, sy))
        if f == 0:
            last = core_tile(data, f3w, fact_in, get_sel, tsel)
    both = jnp.concatenate(res, axis=1)
    row = jnp.concatenate([both[0:8], both[8:16], last], axis=1)
    for d in range(16):
        out[d] = row


def gather_kernel(data, out, sums):
    total = data[0]
    for d in range(1, 16):
        total = total + data[d]
    fact = total[:, 256:384]
    first = pltpu.roll(fact, N - 96, 1)
    lane = lax.broadcasted_iota(jnp.int32, (8, N), 1)
    second = jnp.zeros((8, N), F32)
    for d in range(16):
        moved = pltpu.roll(data[d, :, 256:384], (2 * d - 32) % N, 1)
        second = jnp.where(lane // 2 == d + 16, moved, second)
    sums[...] = jnp.where(lane < 32, first, second)
    tiles = []
    for bh in range(2):
        for q in range(4):
            tile = jnp.zeros((8, N), F32)
            for i in range(4):
                shift = (32 * i - 32 * bh) % N
                moved = data[4 * q + i, :, 256:384]
                moved = pltpu.roll(moved, shift, 1) if shift else moved
                tile = jnp.where(lane // 32 == i, moved, tile)
            tiles.append(tile)
    rows = [
        jnp.concatenate(
            [total[:, h * N : (h + 1) * N]]
            + tiles[2 * h : 2 * h + 2]
            + tiles[2 * h + 4 : 2 * h + 6]
            + [fact],
            axis=1,
        )
        for h in range(2)
    ]
    for d in range(16):
        out[d] = rows[d % 2]


def write_half(data, core, buf, sems, which):
    sends = []
    for q in range(2):
        for d in range(16):
            lo, hi = N + q * N, 3 * N + q * N
            c = jnp.concatenate([data[d, :, lo : lo + N], data[d, :, hi : hi + N]], axis=0)
            rows = slice(d % 2 * 4, d % 2 * 4 + 4)
            buf[4 * q : 4 * q + 4, rows, d // 2] = c.T.reshape(4, 4, 8, 16)
        send = pltpu.make_async_copy(
            buf.at[pl.ds(4 * q, 4)], core.at[pl.ds(8 * which + 4 * q, 4)], sems.at[q]
        )
        send.start()
        sends.append(send)
    return sends


def expand(v, fout, field, obuf, sems):
    row, col = lanes((16, N))
    repeat = marks(row == col % 16)
    choose = sum_y()
    row, col = lanes((512, N))
    hi, lo = [
        jnp.where(row % 8 == col // 16, mul(choose, mul(part, repeat, TN).astype(BF16)), 0.0).astype(BF16)
        for part in split(fout[...])
    ]
    w = jnp.concatenate([hi, hi, lo], axis=1)
    parts = jnp.concatenate([v[0:128], v[128:256], v[0:128]], axis=0)
    puts = []
    for q in range(4):
        u = mul(w[q * 128 : (q + 1) * 128], parts)
        for x in range(8):
            obuf[q * 16 : (q + 1) * 16, x] = u[:, x * N : (x + 1) * N].reshape(16, 8, N).astype(BF16)
        put = pltpu.make_async_copy(
            obuf.at[pl.ds(16 * q, 16)], field.at[pl.ds(16 * q, 16)], sems.at[2 + q]
        )
        put.start()
        puts.append(put)
    return puts


def own_kernel(data, v, fout, sums, core, field, g1, g2, g3, mine, buf, obuf, gbuf, sems):
    sends = write_half(data, core, buf, sems, lax.axis_index("py") % 2)
    total = data[0, :, 0:N]
    for d in range(1, 16):
        total = total + data[d, :, 0:N]
    mine[...] = total
    lane = lanes((8, N))[1]
    third = jnp.zeros((8, N), F32)
    for d in range(16):
        moved = pltpu.roll(data[d, :, 640:768], (2 * d - 66) % N, 1)
        third = jnp.where(lane // 2 == d, moved, third)
    gbuf[0] = sums[:, :32]
    gbuf[1] = sums[:, 32:64]
    gbuf[2] = third[:, :32]
    for i, dst in enumerate((g1, g2, g3)):
        send = pltpu.make_async_copy(gbuf.at[i], dst, sems.at[6 + i])
        send.start()
        sends.append(send)
    sends += expand(v, fout, field, obuf, sems)
    for send in sends:
        send.wait()


def other_kernel(data, mine, core_in, core, gin, gout, buf, gbuf, sems):
    h = lax.axis_index("py") % 2
    sends = write_half(data, core, buf, sems, 1 - h)
    total = data[0, :, 0:N]
    for d in range(1, 16):
        total = total + data[d, :, 0:N]
    own = mine[...]
    for i, rows in enumerate((jnp.where(h == 0, own, total), jnp.where(h == 0, total, own))):
        gbuf[0, 8 * i : 8 * i + 8] = rows[:, :64]
        gbuf[1, 8 * i : 8 * i + 8] = pltpu.roll(rows, 64, 1)[:, :64]
    for i, dst in enumerate((gin, gout)):
        send = pltpu.make_async_copy(gbuf.at[i], dst, sems.at[2 + i])
        send.start()
        sends.append(send)
    for send in sends:
        send.wait()


VM = pl.BlockSpec(memory_space=pltpu.VMEM)
HB = pl.BlockSpec(memory_space=pltpu.HBM)
DMA = pltpu.SemaphoreType.DMA


def call(kernel, ins, outs, scratch=(), flops=1_000_000, vmem=12, aliases=None):
    shapes = [
        pltpu.HBM(*o[:2]) if len(o) > 2 and o[2] is HB
        else jax.ShapeDtypeStruct(*o)
        for o in outs
    ]
    run = pl.pallas_call(
        kernel,
        out_shape=shapes,
        in_specs=[VM] * ins[0] + [HB] * ins[1],
        out_specs=[o[2] if len(o) > 2 else VM for o in outs],
        scratch_shapes=list(scratch),
        input_output_aliases=aliases or {},
        cost_estimate=pl.CostEstimate(flops=flops, bytes_accessed=1_000_000, transcendentals=0),
        compiler_params=pltpu.CompilerParams(vmem_limit_bytes=vmem * 1024 * 1024),
    )

    def placed(*args):
        far = [pltpu.with_memory_space_constraint(v, pltpu.HBM) for v in args[ins[0] :]]
        return run(*args[: ins[0]], *far)

    return placed


def exchange(v, axis):
    return lax.all_to_all(v, axis, split_axis=0, concat_axis=0, tiled=True)


def shards(flow, cot, core, in_factor, out_factor, first, second, third):
    tab = {name: jnp.asarray(value) for name, value in tables().items()}
    fin, fout = in_factor.T, out_factor.T

    o1, yf, fout = call(
        fold_kernel,
        (0, 6),
        [((16, 8, 1024), F32), ((256, 512), BF16), ((16, 64), F32)],
        [
            pltpu.VMEM((2, 64, 8, 8, N), BF16),
            pltpu.VMEM((16, 64), F32),
            pltpu.VMEM((256, 256), BF16),
            pltpu.VMEM((4, 256, 256), F32),
            DMA((13,)),
        ],
    )(flow, cot, fin, fout, tab["zf"], tab["yf"])
    r1 = exchange(o1, "py")
    r1, core, first, second, third = lax.optimization_barrier((r1, core, first, second, third))
    f1t, f2t, f3t = first.T, second.T, third.T
    core_t = core.transpose(0, 2, 3, 4, 1).reshape(16, 512, 16)
    kern, flat, xf, pack, ex, f2w, f3w = call(
        prep_kernel,
        (0, 5),
        [
            ((256, N), F32),
            ((256, 512), F32),
            ((2, 1024, 256), BF16),
            ((32, N), F32),
            ((N, N), F32),
            ((N, N), F32),
            ((N, N), F32),
        ],
        [pltpu.VMEM((8, 32), F32)] * 3 + [pltpu.VMEM((16, 512, 16), F32), DMA((20,))],
        flops=100_000_000,
    )(f1t, f2t, f3t, core_t, tab["xf"])
    o2 = call(y_kernel, (2, 0), [((16, 8, 256), F32)])(r1, yf)[0]
    r2 = exchange(o2, "px")
    o3, gk = call(mode_kernel, (5, 0), [((16, 8, 384), F32), ((256, N), F32)])(
        r2, kern, pack, ex, xf
    )
    r3 = exchange(o3, "px")
    o4, fact = call(unmode_kernel, (6, 0), [((16, 8, 1152), F32), ((8, N), F32)])(
        r3, yf, f2w, gk, flat, pack
    )
    r4 = exchange(o4, "py")
    o5, v = call(
        space_kernel,
        (5, 2),
        [((16, 8, 384), F32), ((256, 1024), BF16)],
        [
            pltpu.VMEM((64, 8, 8, N), BF16),
            pltpu.VMEM((256, 1024), BF16),
            pltpu.VMEM((1024, N), BF16),
            DMA((9,)),
        ],
    )(r4, tab["zf"], f3w, fact, flow, cot, tab["sel"])
    r5 = exchange(o5, "px")
    o6, sums = call(gather_kernel, (1, 0), [((16, 8, 768), F32), ((8, N), F32)])(r5)
    r6 = exchange(o6, "py")
    swapped = lax.ppermute(r6, "py", [(i, i ^ 1) for i in range(16)])
    whole = ((16, 8, 8, 8, 16), F32, HB)
    half = pltpu.VMEM((8, 8, 8, 8, 16), F32)
    small = ((8, 32), F32, HB)
    gcore, field, g1, g2, g3, mine = call(
        own_kernel,
        (4, 0),
        [whole, ((64, 8, 8, N), BF16, HB), small, small, small, ((8, N), F32)],
        [half, pltpu.VMEM((64, 8, 8, N), BF16), pltpu.VMEM((3, 8, 32), F32), DMA((9,))],
        flops=100_000_000,
    )(r6, v, fout, sums)
    small = ((16, 64), F32, HB)
    gcore, gin, gout = call(
        other_kernel,
        (2, 1),
        [whole, small, small],
        [half, pltpu.VMEM((2, 16, 64), F32), DMA((4,))],
        aliases={2: 0},
    )(swapped, mine, gcore)
    return (field, gcore.transpose(0, 4, 1, 2, 3), gin.T, gout.T, g1.T, g2.T, g3.T)


def solution(mesh):
    spec = P(None, "px", "py", None)
    return jax.shard_map(
        shards,
        mesh=mesh,
        in_specs=(spec, spec, P(), P(), P(), P(), P(), P()),
        out_specs=(spec, P(), P(), P(), P(), P(), P()),
        check_vma=False,
    )
```

```python
import functools

import jax
import jax.numpy as jnp
import numpy as np
from jax import lax
from jax.experimental import pallas as pl
from jax.experimental.pallas import tpu as pltpu
from jax.sharding import PartitionSpec as P

N = 128
F32 = jnp.float32
BF16 = jnp.bfloat16
NN = (((1,), (0,)), ((), ()))
NT = (((1,), (1,)), ((), ()))
TN = (((0,), (0,)), ((), ()))


def freq(k):
    return np.where(k < 16, k, k - 32)


def turn(phase, sign):
    angle = 2.0 * np.pi / N * np.mod(phase, N)
    c, s = np.cos(angle), sign * np.sin(angle)
    return np.stack([np.stack([c, s]), np.stack([-s, c])])


def split_table(table):
    hi = np.asarray(table, np.float32).astype(jnp.bfloat16)
    lo = (table - hi.astype(np.float64)).astype(np.float32).astype(jnp.bfloat16)
    return hi, lo


@functools.cache
def tables():
    i2, i8, i16 = np.arange(2), np.arange(8), np.arange(16)
    e2 = np.eye(2)
    z = np.arange(N)
    m = 2 * i16[:, None] + i2[None, :]
    ang = 2.0 * np.pi / N * np.mod(m[:, :, None] * z, N)
    tz = np.stack([np.cos(ang), -np.sin(ang)])
    zf = np.einsum("pdmz,yw->dypmwz", tz, e2).reshape(128, 256)
    k = 2 * i16[:, None] + i2[None, :]
    y = 8 * i16[None, :, None] + 2 * np.arange(4)[:, None, None] + i2[None, None, :]
    ph = freq(k)[:, :, None, None, None] * y[None, None]
    tf = turn(ph, -1.0)
    yf = np.einsum("pqdkgsy,mn->dkmqgsypn", tf, e2).reshape(128, 512)
    x = 8 * i16[None, :] + i8[:, None]
    phx = x[:, :, None] * freq(np.arange(32))[None, None, :]
    tf = turn(phx, -1.0)
    e4 = np.eye(4).reshape(2, 2, 2, 2)
    xf = np.einsum("qrxsj,kmln->xskmqrlnj", tf, e4).reshape(1024, 256)
    sel = np.zeros((8, 128, 2, 2, 4, 8), np.float32)
    for t in range(8):
        for bh in range(2):
            for mm in range(2):
                for r in range(8):
                    sel[t, bh * 16 + mm * 8 + r, r // 4, bh, r % 4, t] = 1.0
    sel = sel.reshape(1024, 128)
    return {
        "zf": np.concatenate(split_table(zf), axis=0),
        "yf": np.concatenate(split_table(yf), axis=0),
        "xf": np.stack(split_table(xf)),
        "sel": sel.astype(jnp.bfloat16),
    }


def split(v):
    hi = v.astype(BF16)
    return hi, (v - hi.astype(F32)).astype(BF16)


def split3(v):
    hi = v.astype(BF16)
    rest = v - hi.astype(F32)
    mid = rest.astype(BF16)
    return hi, mid, (rest - mid.astype(F32)).astype(BF16)


def mul(a, b, dims=NN):
    return lax.dot_general(a, b, dims, preferred_element_type=F32)


def rows_table(table, v, dims=NN):
    half = table.shape[0] // 2
    hi, lo = split(v)
    both = mul(table, hi, dims)
    return both[:half] + both[half:] + mul(table[:half], lo, dims)


def pick(v, table):
    rows = v.shape[0]
    parts = jnp.concatenate([part.astype(F32) for part in split3(v)], axis=0).astype(BF16)
    both = mul(parts, table)
    return both[:rows] + both[rows : 2 * rows] + both[2 * rows :]


def stacked(v, hi, lo, dims=NN):
    axis = 1 if dims is TN else 0
    vh, vl = split(v)
    both = mul(jnp.concatenate([vh, vl], axis=axis), hi, dims)
    half = both.shape[0] // 2
    return both[:half] + both[half:] + mul(vh, lo, dims)


def plane(ref, x):
    return ref[:, x].astype(F32).reshape(512, N).astype(BF16)


def sum_y():
    row, col = lanes((512, 64))
    return marks(row // 8 == col)


def spread(factor, sy):
    row = lax.broadcasted_iota(jnp.int32, (128, 512), 0) // 16
    col = lax.broadcasted_iota(jnp.int32, (128, 512), 1) % 8
    wide = [mul(part, sy, NT) for part in split(factor)]
    return [
        jnp.where(row == col, jnp.concatenate([w] * 8, axis=0), 0.0).astype(BF16) for w in wide
    ]


def fold_kernel(flow, cot, fin, fout, zf, yf, out, yout, tout, fields, tin, tzf, work, sems):
    small = [
        pltpu.make_async_copy(src, dst, sems.at[8 + i])
        for i, (src, dst) in enumerate(((fin, tin), (fout, tout), (zf, tzf)))
    ]
    for copy in small:
        copy.start()
    get_yf = pltpu.make_async_copy(yf, yout, sems.at[12])
    large = []
    for f, field in enumerate((flow, cot)):
        copy = pltpu.make_async_copy(field, fields.at[f], sems.at[f])
        copy.start()
        large.append(copy)
    get_yf.start()
    for copy in small:
        copy.wait()
    sy = sum_y()
    for f, factor in enumerate((tin, tout)):
        w = jnp.concatenate(spread(factor[...], sy), axis=0)
        large[f].wait()
        for pair in range(4):
            u = jnp.concatenate(
                [plane(fields.at[f], 2 * pair), plane(fields.at[f], 2 * pair + 1)], axis=1
            )
            both = mul(w, u)
            v = both[:128] + both[128:]
            for x2 in range(2):
                row = f * 128 + (2 * pair + x2) * 16
                for yy in range(8):
                    work[yy // 2, row : row + 16, (yy % 2) * N : (yy % 2 + 1) * N] = v[
                        yy * 16 : yy * 16 + 16, x2 * N : (x2 + 1) * N
                    ]
    table = tzf[...]
    for g in range(4):
        out[:, :, g * 256 : (g + 1) * 256] = rows_table(table, work[g], NT).reshape(16, 8, 256)
    get_yf.wait()


def y_kernel(data, yf, out):
    v = data[...].reshape(128, 1024)
    v = jnp.concatenate([v[:, g * 256 : (g + 1) * 256] for g in range(4)], axis=0)
    out[...] = rows_table(yf[...], v).reshape(16, 8, 256)


def lanes(shape):
    return lax.broadcasted_iota(jnp.int32, shape, 0), lax.broadcasted_iota(jnp.int32, shape, 1)


def marks(cond):
    return jnp.where(cond, 1.0, 0.0).astype(BF16)


def prep_kernel(
    f1h, f2h, f3h, core, xf, kern, flat, xbuf, pack, ex, f2w, f3w, f1t, f2t, f3t, cbuf, sems
):
    small = [
        pltpu.make_async_copy(src, dst, sems.at[i])
        for i, (src, dst) in enumerate(((f1h, f1t), (f2h, f2t), (f3h, f3t)))
    ]
    loads = [pltpu.make_async_copy(core.at[a], cbuf.at[a], sems.at[4 + a]) for a in range(16)]
    get = pltpu.make_async_copy(xf, xbuf, sems.at[3])
    for copy in small + loads + [get]:
        copy.start()
    for copy in small:
        copy.wait()
    px, py = lax.axis_index("px"), lax.axis_index("py")
    row, lane = lanes((32, N))
    f1 = pick(f1t[...], marks(row == lane % 32))
    f2 = pick(f2t[...], marks(row == 2 * px + lane // 64))
    f3 = pick(f3t[...], marks(row == 2 * py + lane // 32 % 2))
    pack[0:8], pack[8:16], pack[16:24] = f1, f2, f3
    row, lane = lanes((8, N))
    pack[24:32] = jnp.where((py == 0) & (lane // 32 % 2 == 0), 1.0, 2.0) * (1.0 / (N * N * N))
    spread_r = marks(row == lane % 8)
    parts = split3(f1)
    wide = mul(parts[0], spread_r, TN) + mul(parts[1], spread_r, TN) + mul(parts[2], spread_r, TN)
    row, lane = lanes((N, N))
    ex[...] = jnp.where(row // 32 == lane // 8, wide, 0.0)
    w = jnp.concatenate(
        [f1[r : r + 1] * f2[s : s + 1] * f3 for r in range(8) for s in range(8)], axis=0
    )
    row, col = lanes((32, 16 * N))
    block, lane = col // N, col % N
    wide2 = pick(f2t[...], marks(row == 2 * block + lane // 16 % 2))
    wide3 = pick(f3t[...], marks((row == 2 * block + lane // 8 % 2) & (lane < 32)))
    for d in range(16):
        f2w[d * 8 : d * 8 + 8] = wide2[:, d * N : (d + 1) * N]
        f3w[d * 8 : d * 8 + 8] = wide3[:, d * N : (d + 1) * N]
    wh, wl = split(w)
    for a in range(16):
        loads[a].wait()
        flat[a * 16 : (a + 1) * 16, :] = cbuf[a].T
    ch, cl = split(flat[...])
    kern[...] = mul(ch, wh) + mul(cl, wh) + mul(ch, wl)
    get.wait()


def mode_kernel(data, kern, pack, ex, xf, out, gk):
    v = data[...].reshape(128, 256)
    t = [v[:, :128].T, v[:, 128:].T]
    t = jnp.concatenate(
        [jnp.concatenate([part[x * 16 : (x + 1) * 16] for part in t], axis=0) for x in range(8)],
        axis=1,
    )
    s = stacked(t, xf[0], xf[1])
    wt = pack[24:25]
    lift = [s[:16, q * N : (q + 1) * N] for q in range(2)]
    back = [s[16:, q * N : (q + 1) * N] * wt for q in range(2)]
    mixed = [jnp.zeros((16, N), F32) for _ in range(2)]
    lows = [[], []]
    grads = []
    for a in range(16):
        k = kern[a * 16 : (a + 1) * 16]
        g = None
        for q in range(2):
            la = lift[q][a : a + 1]
            mixed[q] = mixed[q] + k * la
            lows[q].append(jnp.sum(k * back[q], axis=0, keepdims=True))
            g = back[q] * la if g is None else g + back[q] * la
        grads.append(g)
    low = [jnp.concatenate(rows, axis=0) for rows in lows]
    gall = jnp.concatenate(grads, axis=0)
    gk[...] = gall
    n = jnp.concatenate(
        [jnp.concatenate([mixed[q] * wt, low[q]], axis=0) for q in range(2)], axis=1
    )
    u = stacked(n, xf[0], xf[1], NT)
    u = jnp.concatenate(
        [
            jnp.concatenate([u[f * 16 : f * 16 + 16, x * N : (x + 1) * N] for x in range(8)], axis=0).T
            for f in range(2)
        ],
        axis=1,
    )
    out[:, :, 0:256] = u.reshape(16, 8, 256)
    gj = stacked(gall, *split(ex[...]))
    gj = gj.reshape(16, 2, 8, N)
    for a in range(16):
        out[a, :, 256:384] = gj[a, 0] + pltpu.roll(gj[a, 1], 64, 1)


def factor_grads(gk, flat, pack):
    gh, gl = split(gk[...])
    ch, cl = split(flat[...])
    gw = mul(jnp.concatenate([ch, cl], axis=0), jnp.concatenate([gh, gh], axis=0), TN) + mul(ch, gl, TN)
    f1, f2, f3 = pack[0:8], pack[8:16], pack[16:24]
    first, second = [None] * 8, [None] * 8
    third = None
    for r in range(8):
        for s in range(8):
            tile = gw[(r * 8 + s) * 8 : (r * 8 + s) * 8 + 8]
            t3 = tile * f3
            one = t3 * f2[s : s + 1]
            two = t3 * f1[r : r + 1]
            tri = tile * (f1[r : r + 1] * f2[s : s + 1])
            first[r] = one if first[r] is None else first[r] + one
            second[s] = two if second[s] is None else second[s] + two
            third = tri if third is None else third + tri
    one = jnp.concatenate([jnp.sum(v, axis=0, keepdims=True) for v in first], axis=0)
    two = jnp.concatenate([jnp.sum(v, axis=0, keepdims=True) for v in second], axis=0)
    src, dst = lanes((N, N))
    total = jnp.zeros((8, N), F32)
    for v, lane in ((one, 96 + src % 32), (two, 64 + src // 64), (third, 66 + src // 32 % 2)):
        total = total + pick(v, marks(dst == lane))
    return total


def unmode_kernel(data, yf, f2w, gk, flat, pack, out, fact):
    hi, lo = split(data[:, :, 0:256].reshape(128, 256))
    u = mul(yf[...], jnp.concatenate([hi, hi], axis=0), TN) + mul(yf[:128], lo, TN)
    for g in range(4):
        out[:, :, g * 256 : (g + 1) * 256] = u[g * 128 : (g + 1) * 128].reshape(16, 8, 256)
    lane = lax.broadcasted_iota(jnp.int32, (8, N), 1)
    extra = factor_grads(gk, flat, pack)
    fact[...] = extra
    for s in range(8):
        acc = jnp.zeros((8, N), F32)
        for d in range(16):
            acc = acc + data[d, :, 256:384] * f2w[d * 8 + s : d * 8 + s + 1]
        acc = acc + pltpu.roll(acc, N - 16, 1)
        acc = jnp.where(lane < 16, acc, pltpu.roll(acc, N - 48, 1))
        acc = jnp.where(lane < 32, acc, extra)
        out[2 * s, :, 1024:1152] = acc
        out[2 * s + 1, :, 1024:1152] = acc


def expand(v, fout, obuf):
    row, col = lanes((16, N))
    repeat = marks(row == col % 16)
    choose = sum_y()
    row, col = lanes((512, N))
    hi, lo = [
        jnp.where(row % 8 == col // 16, mul(choose, mul(part, repeat, TN).astype(BF16)), 0.0).astype(BF16)
        for part in split(fout[...])
    ]
    w = jnp.concatenate([hi, hi, lo], axis=1)
    parts = jnp.concatenate([v[0:128], v[128:256], v[0:128]], axis=0)
    for q in range(4):
        u = mul(w[q * 128 : (q + 1) * 128], parts)
        for x in range(8):
            obuf[q * 16 : (q + 1) * 16, x] = u[:, x * N : (x + 1) * N].reshape(16, 8, N).astype(BF16)


def core_tile(data, f3w, fact_in, get_sel, tsel):
    fact = data[0, :, 1024:1152]
    for d in range(1, 16):
        fact = fact + data[d, :, 1024:1152]
    cols = []
    for t in range(8):
        acc = jnp.zeros((8, N), F32)
        for d in range(16):
            acc = acc + data[d, :, 1024:1152] * f3w[d * 8 + t : d * 8 + t + 1]
        cols.append(acc)
    lane = lanes((8, N))[1]
    get_sel.wait()
    core = pick(jnp.concatenate(cols, axis=1), tsel[...])
    core = jnp.where(lane // 64 == lax.axis_index("py") % 2, core, 0.0)
    core = core + pltpu.roll(core, 64, 1)
    fact = jnp.where((lane == 66) | (lane == 67), fact_in[...], fact)
    return jnp.where(lane < 64, core, fact)


def space_kernel(
    data, zf, f3w, fact_in, flow, fout, cot, sel, out, obuf, vout, second, tsel, sems
):
    sy = sum_y()
    get_sel = pltpu.make_async_copy(sel, tsel, sems.at[1])
    get_sel.start()
    load = pltpu.make_async_copy(cot, second, sems.at[0])
    load.start()
    zl = zf[128:]
    zz = jnp.concatenate([zf[:128], zf[:128]], axis=0)
    for g in range(4):
        v = data[:, :, g * 256 : (g + 1) * 256].reshape(128, 256)
        hi, lo = split(v)
        r = mul(jnp.concatenate([hi, lo], axis=0), zz, TN) + mul(hi, zl, TN)
        rh, rl = split(r)
        for x in range(8):
            for f in range(2):
                for y2 in range(2):
                    row = (2 * g + y2) * 16
                    src = slice(f * 128 + x * 16, f * 128 + x * 16 + 16)
                    cols = slice(y2 * N, (y2 + 1) * N)
                    vout[f, row : row + 16, x * N : (x + 1) * N] = rh[src, cols]
                    vout[f, 128 + row : 128 + row + 16, x * N : (x + 1) * N] = rl[src, cols]
    ri, ci = lanes((128, 512))
    same = ri // 16 == ci % 8
    res = []
    for f, field in enumerate((flow, second)):
        if f == 1:
            load.wait()
        u = jnp.concatenate([plane(field, x) for x in range(8)], axis=1)
        part = mul(vout[1 - f], u, NT)
        p = jnp.where(same, part[:128] + part[128:], 0.0)
        q = p[0:16]
        for yy in range(1, 8):
            q = q + p[yy * 16 : yy * 16 + 16]
        res.append(pick(q, sy))
        if f == 0:
            expand(vout.at[0], fout, obuf)
            last = core_tile(data, f3w, fact_in, get_sel, tsel)
    both = jnp.concatenate(res, axis=1)
    row = jnp.concatenate([both[0:8], both[8:16], last], axis=1)
    for d in range(16):
        out[d] = row


def gather_kernel(data, out, sums):
    total = data[0]
    for d in range(1, 16):
        total = total + data[d]
    fact = total[:, 256:384]
    first = pltpu.roll(fact, N - 96, 1)
    lane = lax.broadcasted_iota(jnp.int32, (8, N), 1)
    second = jnp.zeros((8, N), F32)
    for d in range(16):
        moved = pltpu.roll(data[d, :, 256:384], (2 * d - 32) % N, 1)
        second = jnp.where(lane // 2 == d + 16, moved, second)
    sums[...] = jnp.where(lane < 32, first, second)
    tiles = []
    for bh in range(2):
        for q in range(4):
            tile = jnp.zeros((8, N), F32)
            for i in range(4):
                shift = (32 * i - 32 * bh) % N
                moved = data[4 * q + i, :, 256:384]
                moved = pltpu.roll(moved, shift, 1) if shift else moved
                tile = jnp.where(lane // 32 == i, moved, tile)
            tiles.append(tile)
    rows = [
        jnp.concatenate(
            [total[:, h * N : (h + 1) * N]]
            + tiles[2 * h : 2 * h + 2]
            + tiles[2 * h + 4 : 2 * h + 6]
            + [fact],
            axis=1,
        )
        for h in range(2)
    ]
    for d in range(16):
        out[d] = rows[d % 2]


def write_half(data, core, buf, sems, which):
    sends = []
    for q in range(2):
        for d in range(16):
            lo, hi = N + q * N, 3 * N + q * N
            c = jnp.concatenate([data[d, :, lo : lo + N], data[d, :, hi : hi + N]], axis=0)
            rows = slice(d % 2 * 4, d % 2 * 4 + 4)
            buf[4 * q : 4 * q + 4, rows, d // 2] = c.T.reshape(4, 4, 8, 16)
        send = pltpu.make_async_copy(
            buf.at[pl.ds(4 * q, 4)], core.at[pl.ds(8 * which + 4 * q, 4)], sems.at[q]
        )
        send.start()
        sends.append(send)
    return sends


def own_kernel(data, obuf, sums, core, field, g1, g2, g3, mine, buf, gbuf, sems):
    put = pltpu.make_async_copy(obuf, field, sems.at[2])
    put.start()
    sends = write_half(data, core, buf, sems, lax.axis_index("py") % 2)
    total = data[0, :, 0:N]
    for d in range(1, 16):
        total = total + data[d, :, 0:N]
    mine[...] = total
    lane = lanes((8, N))[1]
    third = jnp.zeros((8, N), F32)
    for d in range(16):
        moved = pltpu.roll(data[d, :, 640:768], (2 * d - 66) % N, 1)
        third = jnp.where(lane // 2 == d, moved, third)
    gbuf[0] = sums[:, :32]
    gbuf[1] = sums[:, 32:64]
    gbuf[2] = third[:, :32]
    for i, dst in enumerate((g1, g2, g3)):
        send = pltpu.make_async_copy(gbuf.at[i], dst, sems.at[3 + i])
        send.start()
        sends.append(send)
    for send in sends + [put]:
        send.wait()


def other_kernel(data, mine, core_in, core, gin, gout, buf, gbuf, sems):
    h = lax.axis_index("py") % 2
    sends = write_half(data, core, buf, sems, 1 - h)
    total = data[0, :, 0:N]
    for d in range(1, 16):
        total = total + data[d, :, 0:N]
    own = mine[...]
    for i, rows in enumerate((jnp.where(h == 0, own, total), jnp.where(h == 0, total, own))):
        gbuf[0, 8 * i : 8 * i + 8] = rows[:, :64]
        gbuf[1, 8 * i : 8 * i + 8] = pltpu.roll(rows, 64, 1)[:, :64]
    for i, dst in enumerate((gin, gout)):
        send = pltpu.make_async_copy(gbuf.at[i], dst, sems.at[2 + i])
        send.start()
        sends.append(send)
    for send in sends:
        send.wait()


VM = pl.BlockSpec(memory_space=pltpu.VMEM)
HB = pl.BlockSpec(memory_space=pltpu.HBM)
DMA = pltpu.SemaphoreType.DMA


def call(kernel, ins, outs, scratch=(), flops=1_000_000, vmem=12, aliases=None):
    shapes = [
        pltpu.HBM(*o[:2]) if len(o) > 2 and o[2] is HB
        else jax.ShapeDtypeStruct(*o)
        for o in outs
    ]
    run = pl.pallas_call(
        kernel,
        out_shape=shapes,
        in_specs=[VM] * ins[0] + [HB] * ins[1],
        out_specs=[o[2] if len(o) > 2 else VM for o in outs],
        scratch_shapes=list(scratch),
        input_output_aliases=aliases or {},
        cost_estimate=pl.CostEstimate(flops=flops, bytes_accessed=1_000_000, transcendentals=0),
        compiler_params=pltpu.CompilerParams(vmem_limit_bytes=vmem * 1024 * 1024),
    )

    def placed(*args):
        far = [pltpu.with_memory_space_constraint(v, pltpu.HBM) for v in args[ins[0] :]]
        return run(*args[: ins[0]], *far)

    return placed


def exchange(v, axis):
    return lax.all_to_all(v, axis, split_axis=0, concat_axis=0, tiled=True)


def shards(flow, cot, core, in_factor, out_factor, first, second, third):
    tab = {name: jnp.asarray(value) for name, value in tables().items()}
    fin, fout = in_factor.T, out_factor.T

    o1, yf, fout = call(
        fold_kernel,
        (0, 6),
        [((16, 8, 1024), F32), ((256, 512), BF16), ((16, 64), F32)],
        [
            pltpu.VMEM((2, 64, 8, 8, N), BF16),
            pltpu.VMEM((16, 64), F32),
            pltpu.VMEM((256, 256), BF16),
            pltpu.VMEM((4, 256, 256), F32),
            DMA((13,)),
        ],
    )(flow, cot, fin, fout, tab["zf"], tab["yf"])
    r1 = exchange(o1, "py")
    r1, core, first, second, third = lax.optimization_barrier((r1, core, first, second, third))
    f1t, f2t, f3t = first.T, second.T, third.T
    core_t = core.transpose(0, 2, 3, 4, 1).reshape(16, 512, 16)
    kern, flat, xf, pack, ex, f2w, f3w = call(
        prep_kernel,
        (0, 5),
        [
            ((256, N), F32),
            ((256, 512), F32),
            ((2, 1024, 256), BF16),
            ((32, N), F32),
            ((N, N), F32),
            ((N, N), F32),
            ((N, N), F32),
        ],
        [pltpu.VMEM((8, 32), F32)] * 3 + [pltpu.VMEM((16, 512, 16), F32), DMA((20,))],
        flops=100_000_000,
    )(f1t, f2t, f3t, core_t, tab["xf"])
    o2 = call(y_kernel, (2, 0), [((16, 8, 256), F32)])(r1, yf)[0]
    r2 = exchange(o2, "px")
    o3, gk = call(mode_kernel, (5, 0), [((16, 8, 384), F32), ((256, N), F32)])(
        r2, kern, pack, ex, xf
    )
    r3 = exchange(o3, "px")
    o4, fact = call(unmode_kernel, (6, 0), [((16, 8, 1152), F32), ((8, N), F32)])(
        r3, yf, f2w, gk, flat, pack
    )
    r4 = exchange(o4, "py")
    o5, obuf = call(
        space_kernel,
        (6, 2),
        [((16, 8, 384), F32), ((64, 8, 8, N), BF16)],
        [
            pltpu.VMEM((2, 256, 1024), BF16),
            pltpu.VMEM((64, 8, 8, N), BF16),
            pltpu.VMEM((1024, N), BF16),
            DMA((2,)),
        ],
    )(r4, tab["zf"], f3w, fact, flow, fout, cot, tab["sel"])
    r5 = exchange(o5, "px")
    o6, sums = call(gather_kernel, (1, 0), [((16, 8, 768), F32), ((8, N), F32)])(r5)
    r6 = exchange(o6, "py")
    swapped = lax.ppermute(r6, "py", [(i, i ^ 1) for i in range(16)])
    whole = ((16, 8, 8, 8, 16), F32, HB)
    half = pltpu.VMEM((8, 8, 8, 8, 16), F32)
    small = ((8, 32), F32, HB)
    gcore, field, g1, g2, g3, mine = call(
        own_kernel,
        (3, 0),
        [whole, ((64, 8, 8, N), BF16, HB), small, small, small, ((8, N), F32)],
        [half, pltpu.VMEM((3, 8, 32), F32), DMA((6,))],
        flops=100_000_000,
    )(r6, obuf, sums)
    small = ((16, 64), F32, HB)
    gcore, gin, gout = call(
        other_kernel,
        (2, 1),
        [whole, small, small],
        [half, pltpu.VMEM((2, 16, 64), F32), DMA((4,))],
        aliases={2: 0},
    )(swapped, mine, gcore)
    return (field, gcore.transpose(0, 4, 1, 2, 3), gin.T, gout.T, g1.T, g2.T, g3.T)


def solution(mesh):
    spec = P(None, "px", "py", None)
    return jax.shard_map(
        shards,
        mesh=mesh,
        in_specs=(spec, spec, P(), P(), P(), P(), P(), P()),
        out_specs=(spec, P(), P(), P(), P(), P(), P()),
        check_vma=False,
    )
```

```python
import functools

import jax
import jax.numpy as jnp
import numpy as np
from jax import lax
from jax.experimental import pallas as pl
from jax.experimental.pallas import tpu as pltpu
from jax.sharding import PartitionSpec as P

N = 128
F32 = jnp.float32
BF16 = jnp.bfloat16
NN = (((1,), (0,)), ((), ()))
NT = (((1,), (1,)), ((), ()))
TN = (((0,), (0,)), ((), ()))


def freq(k):
    return np.where(k < 16, k, k - 32)


def turn(phase, sign):
    angle = 2.0 * np.pi / N * np.mod(phase, N)
    c, s = np.cos(angle), sign * np.sin(angle)
    return np.stack([np.stack([c, s]), np.stack([-s, c])])


def split_table(table):
    hi = np.asarray(table, np.float32).astype(jnp.bfloat16)
    lo = (table - hi.astype(np.float64)).astype(np.float32).astype(jnp.bfloat16)
    return hi, lo


@functools.cache
def tables():
    i2, i8, i16 = np.arange(2), np.arange(8), np.arange(16)
    e2 = np.eye(2)
    z = np.arange(N)
    m = 2 * i16[:, None] + i2[None, :]
    ang = 2.0 * np.pi / N * np.mod(m[:, :, None] * z, N)
    tz = np.stack([np.cos(ang), -np.sin(ang)])
    zf = np.einsum("pdmz,yw->dypmwz", tz, e2).reshape(128, 256)
    k = 2 * i16[:, None] + i2[None, :]
    y = 8 * i16[None, :, None] + 2 * np.arange(4)[:, None, None] + i2[None, None, :]
    ph = freq(k)[:, :, None, None, None] * y[None, None]
    tf = turn(ph, -1.0)
    yf = np.einsum("pqdkgsy,mn->dkmqgsypn", tf, e2).reshape(128, 512)
    x = 8 * i16[None, :] + i8[:, None]
    phx = x[:, :, None] * freq(np.arange(32))[None, None, :]
    tf = turn(phx, -1.0)
    e4 = np.eye(4).reshape(2, 2, 2, 2)
    xf = np.einsum("qrxsj,kmln->xskmqrlnj", tf, e4).reshape(1024, 256)
    sel = np.zeros((8, 128, 2, 2, 4, 8), np.float32)
    for t in range(8):
        for bh in range(2):
            for mm in range(2):
                for r in range(8):
                    sel[t, bh * 16 + mm * 8 + r, r // 4, bh, r % 4, t] = 1.0
    sel = sel.reshape(1024, 128)
    return {
        "zf": np.concatenate(split_table(zf), axis=0),
        "yf": np.concatenate(split_table(yf), axis=0),
        "xf": np.stack(split_table(xf)),
        "sel": sel.astype(jnp.bfloat16),
    }


def split(v):
    hi = v.astype(BF16)
    return hi, (v - hi.astype(F32)).astype(BF16)


def split3(v):
    hi = v.astype(BF16)
    rest = v - hi.astype(F32)
    mid = rest.astype(BF16)
    return hi, mid, (rest - mid.astype(F32)).astype(BF16)


def mul(a, b, dims=NN):
    return lax.dot_general(a, b, dims, preferred_element_type=F32)


def rows_table(table, v, dims=NN):
    half = table.shape[0] // 2
    hi, lo = split(v)
    both = mul(table, hi, dims)
    return both[:half] + both[half:] + mul(table[:half], lo, dims)


def pick(v, table):
    rows = v.shape[0]
    parts = jnp.concatenate([part.astype(F32) for part in split3(v)], axis=0).astype(BF16)
    both = mul(parts, table)
    return both[:rows] + both[rows : 2 * rows] + both[2 * rows :]


def stacked(v, hi, lo, dims=NN):
    axis = 1 if dims is TN else 0
    vh, vl = split(v)
    both = mul(jnp.concatenate([vh, vl], axis=axis), hi, dims)
    half = both.shape[0] // 2
    return both[:half] + both[half:] + mul(vh, lo, dims)


def plane(ref, x):
    return ref[:, x].astype(F32).reshape(512, N).astype(BF16)


def sum_y():
    row, col = lanes((512, 64))
    return marks(row // 8 == col)


def spread(factor, sy):
    row = lax.broadcasted_iota(jnp.int32, (128, 512), 0) // 16
    col = lax.broadcasted_iota(jnp.int32, (128, 512), 1) % 8
    wide = [mul(part, sy, NT) for part in split(factor)]
    return [
        jnp.where(row == col, jnp.concatenate([w] * 8, axis=0), 0.0).astype(BF16) for w in wide
    ]


def fold_kernel(flow, cot, fin, fout, zf, yf, out, yout, tout, fields, tin, tzf, work, sems):
    small = [
        pltpu.make_async_copy(src, dst, sems.at[8 + i])
        for i, (src, dst) in enumerate(((fin, tin), (fout, tout), (zf, tzf)))
    ]
    for copy in small:
        copy.start()
    get_yf = pltpu.make_async_copy(yf, yout, sems.at[12])
    large = []
    for f, field in enumerate((flow, cot)):
        copy = pltpu.make_async_copy(field, fields.at[f], sems.at[f])
        copy.start()
        large.append(copy)
    get_yf.start()
    for copy in small:
        copy.wait()
    sy = sum_y()
    weights = [jnp.concatenate(spread(factor[...], sy), axis=0) for factor in (tin, tout)]
    for f, w in enumerate(weights):
        large[f].wait()
        for pair in range(4):
            u = jnp.concatenate(
                [plane(fields.at[f], 2 * pair), plane(fields.at[f], 2 * pair + 1)], axis=1
            )
            both = mul(w, u)
            v = both[:128] + both[128:]
            for x2 in range(2):
                row = f * 128 + (2 * pair + x2) * 16
                for yy in range(8):
                    work[yy // 2, row : row + 16, (yy % 2) * N : (yy % 2 + 1) * N] = v[
                        yy * 16 : yy * 16 + 16, x2 * N : (x2 + 1) * N
                    ]
    table = tzf[...]
    for g in range(4):
        out[:, :, g * 256 : (g + 1) * 256] = rows_table(table, work[g], NT).reshape(16, 8, 256)
    get_yf.wait()


def y_kernel(data, yf, out):
    v = data[...].reshape(128, 1024)
    v = jnp.concatenate([v[:, g * 256 : (g + 1) * 256] for g in range(4)], axis=0)
    out[...] = rows_table(yf[...], v).reshape(16, 8, 256)


def lanes(shape):
    return lax.broadcasted_iota(jnp.int32, shape, 0), lax.broadcasted_iota(jnp.int32, shape, 1)


def marks(cond):
    return jnp.where(cond, 1.0, 0.0).astype(BF16)


def prep_kernel(
    f1h, f2h, f3h, core, xf, kern, flat, xbuf, pack, ex, f2w, f3w, f1t, f2t, f3t, cbuf, sems
):
    small = [
        pltpu.make_async_copy(src, dst, sems.at[i])
        for i, (src, dst) in enumerate(((f1h, f1t), (f2h, f2t), (f3h, f3t)))
    ]
    loads = [pltpu.make_async_copy(core.at[a], cbuf.at[a], sems.at[4 + a]) for a in range(16)]
    get = pltpu.make_async_copy(xf, xbuf, sems.at[3])
    for copy in small + loads + [get]:
        copy.start()
    for copy in small:
        copy.wait()
    px, py = lax.axis_index("px"), lax.axis_index("py")
    row, lane = lanes((32, N))
    f1 = pick(f1t[...], marks(row == lane % 32))
    f2 = pick(f2t[...], marks(row == 2 * px + lane // 64))
    f3 = pick(f3t[...], marks(row == 2 * py + lane // 32 % 2))
    pack[0:8], pack[8:16], pack[16:24] = f1, f2, f3
    row, lane = lanes((8, N))
    pack[24:32] = jnp.where((py == 0) & (lane // 32 % 2 == 0), 1.0, 2.0) * (1.0 / (N * N * N))
    spread_r = marks(row == lane % 8)
    parts = split3(f1)
    wide = mul(parts[0], spread_r, TN) + mul(parts[1], spread_r, TN) + mul(parts[2], spread_r, TN)
    row, lane = lanes((N, N))
    ex[...] = jnp.where(row // 32 == lane // 8, wide, 0.0)
    w = jnp.concatenate(
        [f1[r : r + 1] * f2[s : s + 1] * f3 for r in range(8) for s in range(8)], axis=0
    )
    row, col = lanes((32, 16 * N))
    block, lane = col // N, col % N
    wide2 = pick(f2t[...], marks(row == 2 * block + lane // 16 % 2))
    wide3 = pick(f3t[...], marks((row == 2 * block + lane // 8 % 2) & (lane < 32)))
    for d in range(16):
        f2w[d * 8 : d * 8 + 8] = wide2[:, d * N : (d + 1) * N]
        f3w[d * 8 : d * 8 + 8] = wide3[:, d * N : (d + 1) * N]
    wh, wl = split(w)
    for a in range(16):
        loads[a].wait()
        flat[a * 16 : (a + 1) * 16, :] = cbuf[a].T
    kern[...] = stacked(flat[...], wh, wl)
    get.wait()


def mode_kernel(data, kern, pack, ex, xf, out, gk):
    v = data[...].reshape(128, 256)
    t = [v[:, :128].T, v[:, 128:].T]
    t = jnp.concatenate(
        [jnp.concatenate([part[x * 16 : (x + 1) * 16] for part in t], axis=0) for x in range(8)],
        axis=1,
    )
    s = stacked(t, xf[0], xf[1])
    wt = pack[24:25]
    lift = [s[:16, q * N : (q + 1) * N] for q in range(2)]
    back = [s[16:, q * N : (q + 1) * N] * wt for q in range(2)]
    mixed = [jnp.zeros((16, N), F32) for _ in range(2)]
    lows = [[], []]
    grads = []
    for a in range(16):
        k = kern[a * 16 : (a + 1) * 16]
        g = None
        for q in range(2):
            la = lift[q][a : a + 1]
            mixed[q] = mixed[q] + k * la
            lows[q].append(jnp.sum(k * back[q], axis=0, keepdims=True))
            g = back[q] * la if g is None else g + back[q] * la
        grads.append(g)
    low = [jnp.concatenate(rows, axis=0) for rows in lows]
    gall = jnp.concatenate(grads, axis=0)
    gk[...] = gall
    n = jnp.concatenate(
        [jnp.concatenate([mixed[q] * wt, low[q]], axis=0) for q in range(2)], axis=1
    )
    u = stacked(n, xf[0], xf[1], NT)
    u = jnp.concatenate(
        [
            jnp.concatenate([u[f * 16 : f * 16 + 16, x * N : (x + 1) * N] for x in range(8)], axis=0).T
            for f in range(2)
        ],
        axis=1,
    )
    out[:, :, 0:256] = u.reshape(16, 8, 256)
    gj = stacked(gall, *split(ex[...]))
    gj = gj.reshape(16, 2, 8, N)
    for a in range(16):
        out[a, :, 256:384] = gj[a, 0] + pltpu.roll(gj[a, 1], 64, 1)


def factor_grads(gk, flat, pack):
    gh, gl = split(gk[...])
    ch, cl = split(flat[...])
    gw = mul(jnp.concatenate([ch, cl], axis=0), jnp.concatenate([gh, gh], axis=0), TN) + mul(ch, gl, TN)
    f1, f2, f3 = pack[0:8], pack[8:16], pack[16:24]
    first, second = [None] * 8, [None] * 8
    third = None
    for r in range(8):
        for s in range(8):
            tile = gw[(r * 8 + s) * 8 : (r * 8 + s) * 8 + 8]
            t3 = tile * f3
            one = t3 * f2[s : s + 1]
            two = t3 * f1[r : r + 1]
            tri = tile * (f1[r : r + 1] * f2[s : s + 1])
            first[r] = one if first[r] is None else first[r] + one
            second[s] = two if second[s] is None else second[s] + two
            third = tri if third is None else third + tri
    one = jnp.concatenate([jnp.sum(v, axis=0, keepdims=True) for v in first], axis=0)
    two = jnp.concatenate([jnp.sum(v, axis=0, keepdims=True) for v in second], axis=0)
    src, dst = lanes((N, N))
    total = jnp.zeros((8, N), F32)
    for v, lane in ((one, 96 + src % 32), (two, 64 + src // 64), (third, 66 + src // 32 % 2)):
        total = total + pick(v, marks(dst == lane))
    return total


def unmode_kernel(data, yf, f2w, gk, flat, pack, out, fact):
    hi, lo = split(data[:, :, 0:256].reshape(128, 256))
    u = mul(yf[...], jnp.concatenate([hi, hi], axis=0), TN) + mul(yf[:128], lo, TN)
    for g in range(4):
        out[:, :, g * 256 : (g + 1) * 256] = u[g * 128 : (g + 1) * 128].reshape(16, 8, 256)
    lane = lax.broadcasted_iota(jnp.int32, (8, N), 1)
    extra = factor_grads(gk, flat, pack)
    fact[...] = extra
    for s in range(8):
        acc = jnp.zeros((8, N), F32)
        for d in range(16):
            acc = acc + data[d, :, 256:384] * f2w[d * 8 + s : d * 8 + s + 1]
        acc = acc + pltpu.roll(acc, N - 16, 1)
        acc = jnp.where(lane < 16, acc, pltpu.roll(acc, N - 48, 1))
        acc = jnp.where(lane < 32, acc, extra)
        out[2 * s, :, 1024:1152] = acc
        out[2 * s + 1, :, 1024:1152] = acc


def expand(v, fout, obuf):
    row, col = lanes((16, N))
    repeat = marks(row == col % 16)
    choose = sum_y()
    row, col = lanes((512, N))
    hi, lo = [
        jnp.where(row % 8 == col // 16, mul(choose, mul(part, repeat, TN).astype(BF16)), 0.0).astype(BF16)
        for part in split(fout[...])
    ]
    w = jnp.concatenate([hi, hi, lo], axis=1)
    parts = jnp.concatenate([v[0:128], v[128:256], v[0:128]], axis=0)
    for q in range(4):
        u = mul(w[q * 128 : (q + 1) * 128], parts)
        for x in range(8):
            obuf[q * 16 : (q + 1) * 16, x] = u[:, x * N : (x + 1) * N].reshape(16, 8, N).astype(BF16)


def core_tile(data, f3w, fact_in, get_sel, tsel):
    fact = data[0, :, 1024:1152]
    for d in range(1, 16):
        fact = fact + data[d, :, 1024:1152]
    cols = []
    for t in range(8):
        acc = jnp.zeros((8, N), F32)
        for d in range(16):
            acc = acc + data[d, :, 1024:1152] * f3w[d * 8 + t : d * 8 + t + 1]
        cols.append(acc)
    lane = lanes((8, N))[1]
    get_sel.wait()
    core = pick(jnp.concatenate(cols, axis=1), tsel[...])
    core = jnp.where(lane // 64 == lax.axis_index("py") % 2, core, 0.0)
    core = core + pltpu.roll(core, 64, 1)
    fact = jnp.where((lane == 66) | (lane == 67), fact_in[...], fact)
    return jnp.where(lane < 64, core, fact)


def space_kernel(
    data, zf, f3w, fact_in, flow, fout, cot, sel, out, obuf, vout, second, tsel, sems
):
    sy = sum_y()
    loads = [
        pltpu.make_async_copy(cot.at[pl.ds(16 * i, 16)], second.at[pl.ds(16 * i, 16)], sems.at[2 + i])
        for i in range(4)
    ]
    for load in loads:
        load.start()
    get_sel = pltpu.make_async_copy(sel, tsel, sems.at[1])
    get_sel.start()
    zl = zf[128:]
    zz = jnp.concatenate([zf[:128], zf[:128]], axis=0)
    for g in range(4):
        v = data[:, :, g * 256 : (g + 1) * 256].reshape(128, 256)
        hi, lo = split(v)
        r = mul(jnp.concatenate([hi, lo], axis=0), zz, TN) + mul(hi, zl, TN)
        rh, rl = split(r)
        for x in range(8):
            for f in range(2):
                for y2 in range(2):
                    row = (2 * g + y2) * 16
                    src = slice(f * 128 + x * 16, f * 128 + x * 16 + 16)
                    cols = slice(y2 * N, (y2 + 1) * N)
                    vout[f, row : row + 16, x * N : (x + 1) * N] = rh[src, cols]
                    vout[f, 128 + row : 128 + row + 16, x * N : (x + 1) * N] = rl[src, cols]
    ri, ci = lanes((128, 512))
    same = ri // 16 == ci % 8
    res = []
    for f, field in enumerate((flow, second)):
        for load in loads if f else ():
            load.wait()
        u = jnp.concatenate([plane(field, x) for x in range(8)], axis=1)
        part = mul(vout[1 - f], u, NT)
        p = jnp.where(same, part[:128] + part[128:], 0.0)
        q = p[0:16]
        for yy in range(1, 8):
            q = q + p[yy * 16 : yy * 16 + 16]
        res.append(pick(q, sy))
        if f == 0:
            expand(vout.at[0], fout, obuf)
    last = core_tile(data, f3w, fact_in, get_sel, tsel)
    both = jnp.concatenate(res, axis=1)
    row = jnp.concatenate([both[0:8], both[8:16], last], axis=1)
    for d in range(16):
        out[d] = row


def gather_kernel(data, out, sums):
    total = data[0]
    for d in range(1, 16):
        total = total + data[d]
    fact = total[:, 256:384]
    first = pltpu.roll(fact, N - 96, 1)
    lane = lax.broadcasted_iota(jnp.int32, (8, N), 1)
    second = jnp.zeros((8, N), F32)
    for d in range(16):
        moved = pltpu.roll(data[d, :, 256:384], (2 * d - 32) % N, 1)
        second = jnp.where(lane // 2 == d + 16, moved, second)
    sums[...] = jnp.where(lane < 32, first, second)
    tiles = []
    for bh in range(2):
        for q in range(4):
            tile = jnp.zeros((8, N), F32)
            for i in range(4):
                shift = (32 * i - 32 * bh) % N
                moved = data[4 * q + i, :, 256:384]
                moved = pltpu.roll(moved, shift, 1) if shift else moved
                tile = jnp.where(lane // 32 == i, moved, tile)
            tiles.append(tile)
    rows = [
        jnp.concatenate(
            [total[:, h * N : (h + 1) * N]]
            + tiles[2 * h : 2 * h + 2]
            + tiles[2 * h + 4 : 2 * h + 6]
            + [fact],
            axis=1,
        )
        for h in range(2)
    ]
    for d in range(16):
        out[d] = rows[d % 2]


def write_half(data, core, buf, sems, which):
    sends = []
    for q in range(2):
        for d in range(16):
            lo, hi = N + q * N, 3 * N + q * N
            c = jnp.concatenate([data[d, :, lo : lo + N], data[d, :, hi : hi + N]], axis=0)
            rows = slice(d % 2 * 4, d % 2 * 4 + 4)
            buf[4 * q : 4 * q + 4, rows, d // 2] = c.T.reshape(4, 4, 8, 16)
        send = pltpu.make_async_copy(
            buf.at[pl.ds(4 * q, 4)], core.at[pl.ds(8 * which + 4 * q, 4)], sems.at[q]
        )
        send.start()
        sends.append(send)
    return sends


def own_kernel(data, obuf, sums, core, field, g1, g2, g3, mine, buf, gbuf, sems):
    put = pltpu.make_async_copy(obuf, field, sems.at[2])
    put.start()
    sends = write_half(data, core, buf, sems, lax.axis_index("py") % 2)
    total = data[0, :, 0:N]
    for d in range(1, 16):
        total = total + data[d, :, 0:N]
    mine[...] = total
    lane = lanes((8, N))[1]
    third = jnp.zeros((8, N), F32)
    for d in range(16):
        moved = pltpu.roll(data[d, :, 640:768], (2 * d - 66) % N, 1)
        third = jnp.where(lane // 2 == d, moved, third)
    gbuf[0] = sums[:, :32]
    gbuf[1] = sums[:, 32:64]
    gbuf[2] = third[:, :32]
    for i, dst in enumerate((g1, g2, g3)):
        send = pltpu.make_async_copy(gbuf.at[i], dst, sems.at[3 + i])
        send.start()
        sends.append(send)
    for send in sends + [put]:
        send.wait()


def other_kernel(data, mine, core_in, core, gin, gout, buf, gbuf, sems):
    h = lax.axis_index("py") % 2
    sends = write_half(data, core, buf, sems, 1 - h)
    total = data[0, :, 0:N]
    for d in range(1, 16):
        total = total + data[d, :, 0:N]
    own = mine[...]
    for i, rows in enumerate((jnp.where(h == 0, own, total), jnp.where(h == 0, total, own))):
        gbuf[0, 8 * i : 8 * i + 8] = rows[:, :64]
        gbuf[1, 8 * i : 8 * i + 8] = pltpu.roll(rows, 64, 1)[:, :64]
    for i, dst in enumerate((gin, gout)):
        send = pltpu.make_async_copy(gbuf.at[i], dst, sems.at[2 + i])
        send.start()
        sends.append(send)
    for send in sends:
        send.wait()


VM = pl.BlockSpec(memory_space=pltpu.VMEM)
HB = pl.BlockSpec(memory_space=pltpu.HBM)
DMA = pltpu.SemaphoreType.DMA


def call(kernel, ins, outs, scratch=(), flops=1_000_000, vmem=12, aliases=None):
    shapes = [
        pltpu.HBM(*o[:2]) if len(o) > 2 and o[2] is HB
        else jax.ShapeDtypeStruct(*o)
        for o in outs
    ]
    run = pl.pallas_call(
        kernel,
        out_shape=shapes,
        in_specs=[VM] * ins[0] + [HB] * ins[1],
        out_specs=[o[2] if len(o) > 2 else VM for o in outs],
        scratch_shapes=list(scratch),
        input_output_aliases=aliases or {},
        cost_estimate=pl.CostEstimate(flops=flops, bytes_accessed=1_000_000, transcendentals=0),
        compiler_params=pltpu.CompilerParams(vmem_limit_bytes=vmem * 1024 * 1024),
    )

    def placed(*args):
        far = [pltpu.with_memory_space_constraint(v, pltpu.HBM) for v in args[ins[0] :]]
        return run(*args[: ins[0]], *far)

    return placed


def exchange(v, axis):
    return lax.all_to_all(v, axis, split_axis=0, concat_axis=0, tiled=True)


def shards(flow, cot, core, in_factor, out_factor, first, second, third):
    tab = {name: jnp.asarray(value) for name, value in tables().items()}
    fin, fout = in_factor.T, out_factor.T

    o1, yf, fout = call(
        fold_kernel,
        (0, 6),
        [((16, 8, 1024), F32), ((256, 512), BF16), ((16, 64), F32)],
        [
            pltpu.VMEM((2, 64, 8, 8, N), BF16),
            pltpu.VMEM((16, 64), F32),
            pltpu.VMEM((256, 256), BF16),
            pltpu.VMEM((4, 256, 256), F32),
            DMA((13,)),
        ],
    )(flow, cot, fin, fout, tab["zf"], tab["yf"])
    r1 = exchange(o1, "py")
    r1, core, first, second, third = lax.optimization_barrier((r1, core, first, second, third))
    f1t, f2t, f3t = first.T, second.T, third.T
    core_t = core.transpose(0, 2, 3, 4, 1).reshape(16, 512, 16)
    kern, flat, xf, pack, ex, f2w, f3w = call(
        prep_kernel,
        (0, 5),
        [
            ((256, N), F32),
            ((256, 512), F32),
            ((2, 1024, 256), BF16),
            ((32, N), F32),
            ((N, N), F32),
            ((N, N), F32),
            ((N, N), F32),
        ],
        [pltpu.VMEM((8, 32), F32)] * 3 + [pltpu.VMEM((16, 512, 16), F32), DMA((20,))],
        flops=100_000_000,
    )(f1t, f2t, f3t, core_t, tab["xf"])
    o2 = call(y_kernel, (2, 0), [((16, 8, 256), F32)])(r1, yf)[0]
    r2 = exchange(o2, "px")
    o3, gk = call(mode_kernel, (5, 0), [((16, 8, 384), F32), ((256, N), F32)])(
        r2, kern, pack, ex, xf
    )
    r3 = exchange(o3, "px")
    o4, fact = call(unmode_kernel, (6, 0), [((16, 8, 1152), F32), ((8, N), F32)])(
        r3, yf, f2w, gk, flat, pack
    )
    r4 = exchange(o4, "py")
    o5, obuf = call(
        space_kernel,
        (6, 2),
        [((16, 8, 384), F32), ((64, 8, 8, N), BF16)],
        [
            pltpu.VMEM((2, 256, 1024), BF16),
            pltpu.VMEM((64, 8, 8, N), BF16),
            pltpu.VMEM((1024, N), BF16),
            DMA((6,)),
        ],
    )(r4, tab["zf"], f3w, fact, flow, fout, cot, tab["sel"])
    r5 = exchange(o5, "px")
    o6, sums = call(gather_kernel, (1, 0), [((16, 8, 768), F32), ((8, N), F32)])(r5)
    r6 = exchange(o6, "py")
    swapped = lax.ppermute(r6, "py", [(i, i ^ 1) for i in range(16)])
    whole = ((16, 8, 8, 8, 16), F32, HB)
    half = pltpu.VMEM((8, 8, 8, 8, 16), F32)
    small = ((8, 32), F32, HB)
    gcore, field, g1, g2, g3, mine = call(
        own_kernel,
        (3, 0),
        [whole, ((64, 8, 8, N), BF16, HB), small, small, small, ((8, N), F32)],
        [half, pltpu.VMEM((3, 8, 32), F32), DMA((6,))],
        flops=100_000_000,
    )(r6, obuf, sums)
    small = ((16, 64), F32, HB)
    gcore, gin, gout = call(
        other_kernel,
        (2, 1),
        [whole, small, small],
        [half, pltpu.VMEM((2, 16, 64), F32), DMA((4,))],
        aliases={2: 0},
    )(swapped, mine, gcore)
    return (field, gcore.transpose(0, 4, 1, 2, 3), gin.T, gout.T, g1.T, g2.T, g3.T)


def solution(mesh):
    spec = P(None, "px", "py", None)
    return jax.shard_map(
        shards,
        mesh=mesh,
        in_specs=(spec, spec, P(), P(), P(), P(), P(), P()),
        out_specs=(spec, P(), P(), P(), P(), P(), P()),
        check_vma=False,
    )
```

```python
import functools

import jax
import jax.numpy as jnp
import numpy as np
from jax import lax
from jax.experimental import pallas as pl
from jax.experimental.pallas import tpu as pltpu
from jax.sharding import PartitionSpec as P

N = 128
F32 = jnp.float32
BF16 = jnp.bfloat16
NN = (((1,), (0,)), ((), ()))
NT = (((1,), (1,)), ((), ()))
TN = (((0,), (0,)), ((), ()))


def freq(k):
    return np.where(k < 16, k, k - 32)


def turn(phase, sign):
    angle = 2.0 * np.pi / N * np.mod(phase, N)
    c, s = np.cos(angle), sign * np.sin(angle)
    return np.stack([np.stack([c, s]), np.stack([-s, c])])


def split_table(table):
    hi = np.asarray(table, np.float32).astype(jnp.bfloat16)
    lo = (table - hi.astype(np.float64)).astype(np.float32).astype(jnp.bfloat16)
    return hi, lo


@functools.cache
def tables():
    i2, i8, i16 = np.arange(2), np.arange(8), np.arange(16)
    e2 = np.eye(2)
    z = np.arange(N)
    m = 2 * i16[:, None] + i2[None, :]
    ang = 2.0 * np.pi / N * np.mod(m[:, :, None] * z, N)
    tz = np.stack([np.cos(ang), -np.sin(ang)])
    zf = np.einsum("pdmz,yw->dypmwz", tz, e2).reshape(128, 256)
    k = 2 * i16[:, None] + i2[None, :]
    y = 8 * i16[None, :, None] + 2 * np.arange(4)[:, None, None] + i2[None, None, :]
    ph = freq(k)[:, :, None, None, None] * y[None, None]
    tf = turn(ph, -1.0)
    yf = np.einsum("pqdkgsy,mn->dkmqgsypn", tf, e2).reshape(128, 512)
    x = 8 * i16[None, :] + i8[:, None]
    phx = x[:, :, None] * freq(np.arange(32))[None, None, :]
    tf = turn(phx, -1.0)
    e4 = np.eye(4).reshape(2, 2, 2, 2)
    xf = np.einsum("qrxsj,kmln->xskmqrlnj", tf, e4).reshape(1024, 256)
    sel = np.zeros((8, 128, 2, 2, 4, 8), np.float32)
    for t in range(8):
        for bh in range(2):
            for mm in range(2):
                for r in range(8):
                    sel[t, bh * 16 + mm * 8 + r, r // 4, bh, r % 4, t] = 1.0
    sel = sel.reshape(1024, 128)
    return {
        "zf": np.concatenate(split_table(zf), axis=0),
        "yf": np.concatenate(split_table(yf), axis=0),
        "xf": np.stack(split_table(xf)),
        "sel": sel.astype(jnp.bfloat16),
    }


def split(v):
    hi = v.astype(BF16)
    return hi, (v - hi.astype(F32)).astype(BF16)


def split3(v):
    hi = v.astype(BF16)
    rest = v - hi.astype(F32)
    mid = rest.astype(BF16)
    return hi, mid, (rest - mid.astype(F32)).astype(BF16)


def mul(a, b, dims=NN):
    return lax.dot_general(a, b, dims, preferred_element_type=F32)


def rows_table(table, v, dims=NN):
    half = table.shape[0] // 2
    hi, lo = split(v)
    both = mul(table, hi, dims)
    return both[:half] + both[half:] + mul(table[:half], lo, dims)


def pick(v, table):
    rows = v.shape[0]
    parts = jnp.concatenate([part.astype(F32) for part in split3(v)], axis=0).astype(BF16)
    both = mul(parts, table)
    return both[:rows] + both[rows : 2 * rows] + both[2 * rows :]


def stacked(v, hi, lo, dims=NN):
    axis = 1 if dims is TN else 0
    vh, vl = split(v)
    both = mul(jnp.concatenate([vh, vl], axis=axis), hi, dims)
    half = both.shape[0] // 2
    return both[:half] + both[half:] + mul(vh, lo, dims)


def plane(ref, x):
    return ref[:, x].astype(F32).reshape(512, N).astype(BF16)


def sum_y():
    row, col = lanes((512, 64))
    return marks(row // 8 == col)


def spread(factor, sy):
    row = lax.broadcasted_iota(jnp.int32, (128, 512), 0) // 16
    col = lax.broadcasted_iota(jnp.int32, (128, 512), 1) % 8
    wide = [mul(part, sy, NT) for part in split(factor)]
    return [
        jnp.where(row == col, jnp.concatenate([w] * 8, axis=0), 0.0).astype(BF16) for w in wide
    ]


def fold_kernel(flow, cot, fin, fout, zf, yf, out, yout, tout, fields, tin, tzf, work, sems):
    small = [
        pltpu.make_async_copy(src, dst, sems.at[8 + i])
        for i, (src, dst) in enumerate(((fin, tin), (fout, tout), (zf, tzf)))
    ]
    for copy in small:
        copy.start()
    get_yf = pltpu.make_async_copy(yf, yout, sems.at[12])
    large = []
    for f, field in enumerate((flow, cot)):
        copy = pltpu.make_async_copy(field, fields.at[f], sems.at[f])
        copy.start()
        large.append(copy)
    get_yf.start()
    for copy in small:
        copy.wait()
    sy = sum_y()
    weights = [jnp.concatenate(spread(factor[...], sy), axis=0) for factor in (tin, tout)]
    for f, w in enumerate(weights):
        large[f].wait()
        for pair in range(4):
            u = jnp.concatenate(
                [plane(fields.at[f], 2 * pair), plane(fields.at[f], 2 * pair + 1)], axis=1
            )
            both = mul(w, u)
            v = both[:128] + both[128:]
            for x2 in range(2):
                row = f * 128 + (2 * pair + x2) * 16
                for yy in range(8):
                    work[yy // 2, row : row + 16, (yy % 2) * N : (yy % 2 + 1) * N] = v[
                        yy * 16 : yy * 16 + 16, x2 * N : (x2 + 1) * N
                    ]
    table = tzf[...]
    for g in range(4):
        out[:, :, g * 256 : (g + 1) * 256] = rows_table(table, work[g], NT).reshape(16, 8, 256)
    get_yf.wait()


def y_kernel(data, yf, out):
    v = data[...].reshape(128, 1024)
    v = jnp.concatenate([v[:, g * 256 : (g + 1) * 256] for g in range(4)], axis=0)
    out[...] = rows_table(yf[...], v).reshape(16, 8, 256)


def lanes(shape):
    return lax.broadcasted_iota(jnp.int32, shape, 0), lax.broadcasted_iota(jnp.int32, shape, 1)


def marks(cond):
    return jnp.where(cond, 1.0, 0.0).astype(BF16)


def prep_kernel(
    f1h, f2h, f3h, core, xf, kern, flat, xbuf, pack, ex, f2w, f3w, f1t, f2t, f3t, cbuf, sems
):
    small = [
        pltpu.make_async_copy(src, dst, sems.at[i])
        for i, (src, dst) in enumerate(((f1h, f1t), (f2h, f2t), (f3h, f3t)))
    ]
    loads = [pltpu.make_async_copy(core.at[a], cbuf.at[a], sems.at[4 + a]) for a in range(16)]
    get = pltpu.make_async_copy(xf, xbuf, sems.at[3])
    for copy in small + loads + [get]:
        copy.start()
    for copy in small:
        copy.wait()
    px, py = lax.axis_index("px"), lax.axis_index("py")
    row, lane = lanes((32, N))
    f1 = pick(f1t[...], marks(row == lane % 32))
    f2 = pick(f2t[...], marks(row == 2 * px + lane // 64))
    f3 = pick(f3t[...], marks(row == 2 * py + lane // 32 % 2))
    pack[0:8], pack[8:16], pack[16:24] = f1, f2, f3
    row, lane = lanes((8, N))
    pack[24:32] = jnp.where((py == 0) & (lane // 32 % 2 == 0), 1.0, 2.0) * (1.0 / (N * N * N))
    spread_r = marks(row == lane % 8)
    parts = split3(f1)
    wide = mul(parts[0], spread_r, TN) + mul(parts[1], spread_r, TN) + mul(parts[2], spread_r, TN)
    row, lane = lanes((N, N))
    ex[...] = jnp.where(row // 32 == lane // 8, wide, 0.0)
    w = jnp.concatenate(
        [f1[r : r + 1] * f2[s : s + 1] * f3 for r in range(8) for s in range(8)], axis=0
    )
    row, lane = lanes((N, N))
    zero = jnp.zeros((8, 96), F32)
    for src, dst, where in (
        (f2t, f2w, row == lane // 16 % 2),
        (f3t, f3w, (row == lane // 8 % 2) & (lane < 32)),
    ):
        wide = jnp.concatenate([src[...], zero], axis=1)
        moved = [wide] + [pltpu.roll(wide, N - 2 * d, 1) for d in range(1, 16)]
        dst[...] = pick(jnp.concatenate(moved, axis=0), marks(where))
    wh, wl = split(w)
    for a in range(16):
        loads[a].wait()
        flat[a * 16 : (a + 1) * 16, :] = cbuf[a].T
    kern[...] = stacked(flat[...], wh, wl)
    get.wait()


def mode_kernel(data, kern, pack, ex, xf, out, gk):
    v = data[...].reshape(128, 256)
    t = [v[:, :128].T, v[:, 128:].T]
    t = jnp.concatenate(
        [jnp.concatenate([part[x * 16 : (x + 1) * 16] for part in t], axis=0) for x in range(8)],
        axis=1,
    )
    s = stacked(t, xf[0], xf[1])
    wt = pack[24:25]
    lift = [s[:16, q * N : (q + 1) * N] for q in range(2)]
    back = [s[16:, q * N : (q + 1) * N] * wt for q in range(2)]
    mixed = [jnp.zeros((16, N), F32) for _ in range(2)]
    lows = [[], []]
    grads = []
    for a in range(16):
        k = kern[a * 16 : (a + 1) * 16]
        g = None
        for q in range(2):
            la = lift[q][a : a + 1]
            mixed[q] = mixed[q] + k * la
            lows[q].append(jnp.sum(k * back[q], axis=0, keepdims=True))
            g = back[q] * la if g is None else g + back[q] * la
        grads.append(g)
    low = [jnp.concatenate(rows, axis=0) for rows in lows]
    gall = jnp.concatenate(grads, axis=0)
    gk[...] = gall
    n = jnp.concatenate(
        [jnp.concatenate([mixed[q] * wt, low[q]], axis=0) for q in range(2)], axis=1
    )
    u = stacked(n, xf[0], xf[1], NT)
    u = jnp.concatenate(
        [
            jnp.concatenate([u[f * 16 : f * 16 + 16, x * N : (x + 1) * N] for x in range(8)], axis=0).T
            for f in range(2)
        ],
        axis=1,
    )
    out[:, :, 0:256] = u.reshape(16, 8, 256)
    gj = stacked(gall, *split(ex[...]))
    gj = gj.reshape(16, 2, 8, N)
    for a in range(16):
        out[a, :, 256:384] = gj[a, 0] + pltpu.roll(gj[a, 1], 64, 1)


def factor_grads(gk, flat, pack):
    gh, gl = split(gk[...])
    ch, cl = split(flat[...])
    gw = mul(jnp.concatenate([ch, cl], axis=0), jnp.concatenate([gh, gh], axis=0), TN) + mul(ch, gl, TN)
    f1, f2, f3 = pack[0:8], pack[8:16], pack[16:24]
    first, second = [None] * 8, [None] * 8
    third = None
    for r in range(8):
        for s in range(8):
            tile = gw[(r * 8 + s) * 8 : (r * 8 + s) * 8 + 8]
            t3 = tile * f3
            one = t3 * f2[s : s + 1]
            two = t3 * f1[r : r + 1]
            tri = tile * (f1[r : r + 1] * f2[s : s + 1])
            first[r] = one if first[r] is None else first[r] + one
            second[s] = two if second[s] is None else second[s] + two
            third = tri if third is None else third + tri
    one = jnp.concatenate([jnp.sum(v, axis=0, keepdims=True) for v in first], axis=0)
    two = jnp.concatenate([jnp.sum(v, axis=0, keepdims=True) for v in second], axis=0)
    src, dst = lanes((N, N))
    total = jnp.zeros((8, N), F32)
    for v, lane in ((one, 96 + src % 32), (two, 64 + src // 64), (third, 66 + src // 32 % 2)):
        total = total + pick(v, marks(dst == lane))
    return total


def unmode_kernel(data, yf, f2w, gk, flat, pack, out, fact):
    hi, lo = split(data[:, :, 0:256].reshape(128, 256))
    u = mul(yf[...], jnp.concatenate([hi, hi], axis=0), TN) + mul(yf[:128], lo, TN)
    for g in range(4):
        out[:, :, g * 256 : (g + 1) * 256] = u[g * 128 : (g + 1) * 128].reshape(16, 8, 256)
    lane = lax.broadcasted_iota(jnp.int32, (8, N), 1)
    extra = factor_grads(gk, flat, pack)
    fact[...] = extra
    for s in range(8):
        acc = jnp.zeros((8, N), F32)
        for d in range(16):
            acc = acc + data[d, :, 256:384] * f2w[d * 8 + s : d * 8 + s + 1]
        acc = acc + pltpu.roll(acc, N - 16, 1)
        acc = jnp.where(lane < 16, acc, pltpu.roll(acc, N - 48, 1))
        acc = jnp.where(lane < 32, acc, extra)
        out[2 * s, :, 1024:1152] = acc
        out[2 * s + 1, :, 1024:1152] = acc


def expand(v, fout, obuf):
    row, col = lanes((16, N))
    repeat = marks(row == col % 16)
    choose = sum_y()
    row, col = lanes((512, N))
    hi, lo = [
        jnp.where(row % 8 == col // 16, mul(choose, mul(part, repeat, TN).astype(BF16)), 0.0).astype(BF16)
        for part in split(fout[...])
    ]
    w = jnp.concatenate([hi, hi, lo], axis=1)
    parts = jnp.concatenate([v[0:128], v[128:256], v[0:128]], axis=0)
    for q in range(4):
        u = mul(w[q * 128 : (q + 1) * 128], parts)
        for x in range(8):
            obuf[q * 16 : (q + 1) * 16, x] = u[:, x * N : (x + 1) * N].reshape(16, 8, N).astype(BF16)


def core_tile(data, f3w, fact_in, get_sel, tsel):
    fact = data[0, :, 1024:1152]
    for d in range(1, 16):
        fact = fact + data[d, :, 1024:1152]
    cols = []
    for t in range(8):
        acc = jnp.zeros((8, N), F32)
        for d in range(16):
            acc = acc + data[d, :, 1024:1152] * f3w[d * 8 + t : d * 8 + t + 1]
        cols.append(acc)
    lane = lanes((8, N))[1]
    get_sel.wait()
    core = pick(jnp.concatenate(cols, axis=1), tsel[...])
    core = jnp.where(lane // 64 == lax.axis_index("py") % 2, core, 0.0)
    core = core + pltpu.roll(core, 64, 1)
    fact = jnp.where((lane == 66) | (lane == 67), fact_in[...], fact)
    return jnp.where(lane < 64, core, fact)


def space_kernel(
    data, zf, f3w, fact_in, flow, fout, cot, sel, out, obuf, vout, second, tsel, sems
):
    sy = sum_y()
    loads = [
        pltpu.make_async_copy(cot.at[pl.ds(16 * i, 16)], second.at[pl.ds(16 * i, 16)], sems.at[2 + i])
        for i in range(4)
    ]
    for load in loads:
        load.start()
    get_sel = pltpu.make_async_copy(sel, tsel, sems.at[1])
    get_sel.start()
    zl = zf[128:]
    zz = jnp.concatenate([zf[:128], zf[:128]], axis=0)
    for g in range(4):
        v = data[:, :, g * 256 : (g + 1) * 256].reshape(128, 256)
        hi, lo = split(v)
        r = mul(jnp.concatenate([hi, lo], axis=0), zz, TN) + mul(hi, zl, TN)
        rh, rl = split(r)
        for x in range(8):
            for f in range(2):
                for y2 in range(2):
                    row = (2 * g + y2) * 16
                    src = slice(f * 128 + x * 16, f * 128 + x * 16 + 16)
                    cols = slice(y2 * N, (y2 + 1) * N)
                    vout[f, row : row + 16, x * N : (x + 1) * N] = rh[src, cols]
                    vout[f, 128 + row : 128 + row + 16, x * N : (x + 1) * N] = rl[src, cols]
    ri, ci = lanes((128, 512))
    same = ri // 16 == ci % 8
    res = []
    for f, field in enumerate((flow, second)):
        for load in loads if f else ():
            load.wait()
        u = jnp.concatenate([plane(field, x) for x in range(8)], axis=1)
        part = mul(vout[1 - f], u, NT)
        p = jnp.where(same, part[:128] + part[128:], 0.0)
        q = p[0:16]
        for yy in range(1, 8):
            q = q + p[yy * 16 : yy * 16 + 16]
        res.append(pick(q, sy))
        if f == 0:
            expand(vout.at[0], fout, obuf)
    last = core_tile(data, f3w, fact_in, get_sel, tsel)
    both = jnp.concatenate(res, axis=1)
    row = jnp.concatenate([both[0:8], both[8:16], last], axis=1)
    for d in range(16):
        out[d] = row


def gather_kernel(data, out, sums):
    total = data[0]
    for d in range(1, 16):
        total = total + data[d]
    fact = total[:, 256:384]
    first = pltpu.roll(fact, N - 96, 1)
    lane = lax.broadcasted_iota(jnp.int32, (8, N), 1)
    second = jnp.zeros((8, N), F32)
    for d in range(16):
        moved = pltpu.roll(data[d, :, 256:384], (2 * d - 32) % N, 1)
        second = jnp.where(lane // 2 == d + 16, moved, second)
    sums[...] = jnp.where(lane < 32, first, second)
    tiles = []
    for bh in range(2):
        for q in range(4):
            tile = jnp.zeros((8, N), F32)
            for i in range(4):
                shift = (32 * i - 32 * bh) % N
                moved = data[4 * q + i, :, 256:384]
                moved = pltpu.roll(moved, shift, 1) if shift else moved
                tile = jnp.where(lane // 32 == i, moved, tile)
            tiles.append(tile)
    rows = [
        jnp.concatenate(
            [total[:, h * N : (h + 1) * N]]
            + tiles[2 * h : 2 * h + 2]
            + tiles[2 * h + 4 : 2 * h + 6]
            + [fact],
            axis=1,
        )
        for h in range(2)
    ]
    for d in range(16):
        out[d] = rows[d % 2]


def write_half(data, core, buf, sems, which):
    sends = []
    for q in range(2):
        for d in range(16):
            lo, hi = N + q * N, 3 * N + q * N
            c = jnp.concatenate([data[d, :, lo : lo + N], data[d, :, hi : hi + N]], axis=0)
            rows = slice(d % 2 * 4, d % 2 * 4 + 4)
            buf[4 * q : 4 * q + 4, rows, d // 2] = c.T.reshape(4, 4, 8, 16)
        send = pltpu.make_async_copy(
            buf.at[pl.ds(4 * q, 4)], core.at[pl.ds(8 * which + 4 * q, 4)], sems.at[q]
        )
        send.start()
        sends.append(send)
    return sends


def own_kernel(data, obuf, sums, core, field, g1, g2, g3, mine, buf, gbuf, sems):
    put = pltpu.make_async_copy(obuf, field, sems.at[2])
    put.start()
    sends = write_half(data, core, buf, sems, lax.axis_index("py") % 2)
    total = data[0, :, 0:N]
    for d in range(1, 16):
        total = total + data[d, :, 0:N]
    mine[...] = total
    lane = lanes((8, N))[1]
    third = jnp.zeros((8, N), F32)
    for d in range(16):
        moved = pltpu.roll(data[d, :, 640:768], (2 * d - 66) % N, 1)
        third = jnp.where(lane // 2 == d, moved, third)
    gbuf[0] = sums[:, :32]
    gbuf[1] = sums[:, 32:64]
    gbuf[2] = third[:, :32]
    for i, dst in enumerate((g1, g2, g3)):
        send = pltpu.make_async_copy(gbuf.at[i], dst, sems.at[3 + i])
        send.start()
        sends.append(send)
    for send in sends + [put]:
        send.wait()


def other_kernel(data, mine, core_in, core, gin, gout, buf, gbuf, sems):
    h = lax.axis_index("py") % 2
    sends = write_half(data, core, buf, sems, 1 - h)
    total = data[0, :, 0:N]
    for d in range(1, 16):
        total = total + data[d, :, 0:N]
    own = mine[...]
    for i, rows in enumerate((jnp.where(h == 0, own, total), jnp.where(h == 0, total, own))):
        gbuf[0, 8 * i : 8 * i + 8] = rows[:, :64]
        gbuf[1, 8 * i : 8 * i + 8] = pltpu.roll(rows, 64, 1)[:, :64]
    for i, dst in enumerate((gin, gout)):
        send = pltpu.make_async_copy(gbuf.at[i], dst, sems.at[2 + i])
        send.start()
        sends.append(send)
    for send in sends:
        send.wait()


VM = pl.BlockSpec(memory_space=pltpu.VMEM)
HB = pl.BlockSpec(memory_space=pltpu.HBM)
DMA = pltpu.SemaphoreType.DMA


def call(kernel, ins, outs, scratch=(), flops=1_000_000, vmem=12, aliases=None):
    shapes = [
        pltpu.HBM(*o[:2]) if len(o) > 2 and o[2] is HB
        else jax.ShapeDtypeStruct(*o)
        for o in outs
    ]
    run = pl.pallas_call(
        kernel,
        out_shape=shapes,
        in_specs=[VM] * ins[0] + [HB] * ins[1],
        out_specs=[o[2] if len(o) > 2 else VM for o in outs],
        scratch_shapes=list(scratch),
        input_output_aliases=aliases or {},
        cost_estimate=pl.CostEstimate(flops=flops, bytes_accessed=1_000_000, transcendentals=0),
        compiler_params=pltpu.CompilerParams(vmem_limit_bytes=vmem * 1024 * 1024),
    )

    def placed(*args):
        far = [pltpu.with_memory_space_constraint(v, pltpu.HBM) for v in args[ins[0] :]]
        return run(*args[: ins[0]], *far)

    return placed


def exchange(v, axis):
    return lax.all_to_all(v, axis, split_axis=0, concat_axis=0, tiled=True)


def shards(flow, cot, core, in_factor, out_factor, first, second, third):
    tab = {name: jnp.asarray(value) for name, value in tables().items()}
    fin, fout = in_factor.T, out_factor.T

    o1, yf, fout = call(
        fold_kernel,
        (0, 6),
        [((16, 8, 1024), F32), ((256, 512), BF16), ((16, 64), F32)],
        [
            pltpu.VMEM((2, 64, 8, 8, N), BF16),
            pltpu.VMEM((16, 64), F32),
            pltpu.VMEM((256, 256), BF16),
            pltpu.VMEM((4, 256, 256), F32),
            DMA((13,)),
        ],
    )(flow, cot, fin, fout, tab["zf"], tab["yf"])
    r1 = exchange(o1, "py")
    r1, core, first, second, third = lax.optimization_barrier((r1, core, first, second, third))
    f1t, f2t, f3t = first.T, second.T, third.T
    core_t = core.transpose(0, 2, 3, 4, 1).reshape(16, 512, 16)
    kern, flat, xf, pack, ex, f2w, f3w = call(
        prep_kernel,
        (0, 5),
        [
            ((256, N), F32),
            ((256, 512), F32),
            ((2, 1024, 256), BF16),
            ((32, N), F32),
            ((N, N), F32),
            ((N, N), F32),
            ((N, N), F32),
        ],
        [pltpu.VMEM((8, 32), F32)] * 3 + [pltpu.VMEM((16, 512, 16), F32), DMA((20,))],
        flops=100_000_000,
    )(f1t, f2t, f3t, core_t, tab["xf"])
    o2 = call(y_kernel, (2, 0), [((16, 8, 256), F32)])(r1, yf)[0]
    r2 = exchange(o2, "px")
    o3, gk = call(mode_kernel, (5, 0), [((16, 8, 384), F32), ((256, N), F32)])(
        r2, kern, pack, ex, xf
    )
    r3 = exchange(o3, "px")
    o4, fact = call(unmode_kernel, (6, 0), [((16, 8, 1152), F32), ((8, N), F32)])(
        r3, yf, f2w, gk, flat, pack
    )
    r4 = exchange(o4, "py")
    o5, obuf = call(
        space_kernel,
        (6, 2),
        [((16, 8, 384), F32), ((64, 8, 8, N), BF16)],
        [
            pltpu.VMEM((2, 256, 1024), BF16),
            pltpu.VMEM((64, 8, 8, N), BF16),
            pltpu.VMEM((1024, N), BF16),
            DMA((6,)),
        ],
    )(r4, tab["zf"], f3w, fact, flow, fout, cot, tab["sel"])
    r5 = exchange(o5, "px")
    o6, sums = call(gather_kernel, (1, 0), [((16, 8, 768), F32), ((8, N), F32)])(r5)
    r6 = exchange(o6, "py")
    swapped = lax.ppermute(r6, "py", [(i, i ^ 1) for i in range(16)])
    whole = ((16, 8, 8, 8, 16), F32, HB)
    half = pltpu.VMEM((8, 8, 8, 8, 16), F32)
    small = ((8, 32), F32, HB)
    gcore, field, g1, g2, g3, mine = call(
        own_kernel,
        (3, 0),
        [whole, ((64, 8, 8, N), BF16, HB), small, small, small, ((8, N), F32)],
        [half, pltpu.VMEM((3, 8, 32), F32), DMA((6,))],
        flops=100_000_000,
    )(r6, obuf, sums)
    small = ((16, 64), F32, HB)
    gcore, gin, gout = call(
        other_kernel,
        (2, 1),
        [whole, small, small],
        [half, pltpu.VMEM((2, 16, 64), F32), DMA((4,))],
        aliases={2: 0},
    )(swapped, mine, gcore)
    return (field, gcore.transpose(0, 4, 1, 2, 3), gin.T, gout.T, g1.T, g2.T, g3.T)


def solution(mesh):
    spec = P(None, "px", "py", None)
    return jax.shard_map(
        shards,
        mesh=mesh,
        in_specs=(spec, spec, P(), P(), P(), P(), P(), P()),
        out_specs=(spec, P(), P(), P(), P(), P(), P()),
        check_vma=False,
    )
```
